32 devices in a mesh: dev: 32 (over z, y, x, core).
Axes of the slice: x: 2, y: 2, z: 4, core: 2. Of those that a mesh axis runs over, the one named last changes fastest.
Arguments:
- embeddings: float32 [8192, 1024], P('dev'), may hold values from -6 to 6
- lists: int32 [8192], P('dev'), may hold values from 0 to 65535, as said below
- row_ids: int32 [8192], P('dev'), may hold values from 0 to 8191, each once
- centroids: float32 [65536, 1024], P('dev'), may hold values from -6 to 6
- rotation: float32 [1024, 1024], replicated, may hold values from -0.1875 to 0.1875
Outputs:
- packed: float32 [16384, 1024], P('dev')
- packed_ids: int32 [16384], P('dev')
- list_offsets: int32 [65536], P('dev')
The draws below stay inside these ranges and needn't reach their ends.
Inputs may be any that keep to these rules, and one draw needn't show every extreme that they name: Lists l * 2048 to (l + 1) * 2048 - 1 belong to owner l. Among the rows of one device, at most 16 have lists of one owner, so an owner receives at most 512 rows; in every draw some owner receives exactly 16 rows from every device. `row_ids`: all identifiers are distinct.
All inputs are finite; a program needn't handle non-finite values.
Results may differ from the reference program's by a relative error of at most 0.0003.
Values sent between devices are 32-bit elements; how exact they have to be, the bound alone decides.
A program may use at most 64 MiB of HBM per device.

```python
import jax
import jax.numpy as jnp
from jax import lax

D = 1024
LISTS = 65536
ROWS_DEV = 256
TOTAL = 8192
LISTS_DEV = 2048
SLOTS = 16
CAP = 512
N_DEV = 32


def draw_lists(key, part):
    full_key = jax.random.fold_in(key, 11)
    crowded = jax.random.randint(full_key, (), 0, N_DEV).astype(jnp.int32)

    def one_block(block_key):
        first_key = jax.random.fold_in(block_key, 1)
        second_key = jax.random.fold_in(block_key, 2)
        third_key = jax.random.fold_in(block_key, 3)
        shuffled = jax.random.permutation(first_key, (N_DEV - 1) * SLOTS).astype(jnp.int32)
        others = shuffled // SLOTS
        others = others + (others >= crowded).astype(jnp.int32)
        owners = jnp.concatenate([jnp.full((SLOTS,), 1, jnp.int32) * crowded, others[:ROWS_DEV - SLOTS]])
        mixing = jax.random.permutation(second_key, ROWS_DEV).astype(jnp.int32)
        owners = owners[mixing]
        inside = jax.random.randint(third_key, (ROWS_DEV,), 0, LISTS_DEV).astype(jnp.int32)
        return owners * LISTS_DEV + inside
    block_keys = jax.random.split(jax.random.fold_in(key, 12), N_DEV)
    return jax.vmap(one_block)(block_keys).reshape(-1).astype(jnp.int32)


def shard_levels(rng, dims, cuts, least, high):
    level = 1.0
    for axis_at, shards_of in cuts:
        steps = jax.random.uniform(jax.random.fold_in(jax.random.fold_in(rng, 6), axis_at), (shards_of,), jnp.float32, least / len(cuts), high / len(cuts))
        level = level * jnp.repeat(jnp.exp(steps), dims[axis_at] // shards_of).reshape((-1,) + (1,) * (len(dims) - 1 - axis_at))
    return level


def centred(own_key, shape, spread, most, cuts=(), held_as=jnp.bfloat16):
    gain = shard_levels(own_key, shape, cuts, -0.22, 0.18) if cuts else 1.0
    array = jax.random.normal(own_key, shape, jnp.float32) * spread * gain
    return jnp.minimum(jnp.maximum(array, -most), most).astype(held_as)


def setup_inputs(seed: int = 0) -> dict:
    key_of = jax.random.split(jax.random.key(seed), 6)
    return {
        "embeddings": centred(key_of[0], (TOTAL, D), 1.0, 6.0, ((0, 32),), jnp.float32),
        "lists": draw_lists(jax.random.fold_in(key_of[5], 71), 0),
        "row_ids": jax.random.permutation(key_of[2], TOTAL).astype(jnp.int32),
        "centroids": centred(key_of[3], (LISTS, D), 1.0, 6.0, ((0, 32),), jnp.float32),
        "rotation": centred(key_of[4], (D, D), D ** -0.5, 0.1875, (), jnp.float32),
    }


def reference(embeddings, lists, row_ids, centroids, rotation):
    total_rows = lists.shape[0]
    residual = embeddings - centroids[lists]
    transformed = jnp.dot(residual, rotation, precision=lax.Precision.HIGHEST, preferred_element_type=jnp.float32)
    sorted_order = jnp.argsort(lists, stable=True).astype(jnp.int32)
    sorted_lists = lists[sorted_order]
    owner_sorted = (sorted_lists // LISTS_DEV).astype(jnp.int32)
    owner_counts = jnp.zeros((N_DEV,), jnp.int32).at[owner_sorted].add(1)
    owner_first = (jnp.cumsum(owner_counts) - owner_counts).astype(jnp.int32)
    positions = jnp.arange(total_rows, dtype=jnp.int32) - owner_first[owner_sorted]
    destination = (owner_sorted * CAP + positions).astype(jnp.int32)
    packed = jnp.zeros((N_DEV * CAP, D), jnp.float32).at[destination].set(transformed[sorted_order])
    packed_ids = jnp.full((N_DEV * CAP,), -1, jnp.int32).at[destination].set(row_ids[sorted_order])
    totals = jnp.zeros((LISTS,), jnp.int32).at[lists].add(1)
    tiled_totals = totals.reshape(N_DEV, LISTS_DEV)
    list_offsets = (jnp.cumsum(tiled_totals, axis=1) - tiled_totals).reshape(-1).astype(jnp.int32)
    return packed, packed_ids, list_offsets
```

```python
import functools

import jax
import jax.numpy as jnp
from jax import lax
from jax.experimental import pallas as pl
from jax.experimental.pallas import tpu as pltpu
from jax.sharding import PartitionSpec as P

MESH = pl.DeviceIdType.MESH
F32 = jnp.float32
BF16 = jnp.bfloat16
LANES = 128


def split(x):
    hi = x.astype(BF16)
    lo = (x - hi.astype(F32)).astype(BF16)
    return hi, lo


def dot(a, b):
    return jnp.dot(a, b, preferred_element_type=F32)


def kernel(
    n, slots, chunks,
    send, meta, cent, rot,
    out, ids_out, off_out,
    recv, meta_in, cent_buf, rot_buf, rot_hi, rot_lo, res, place,
    send_sem, recv_sem, meta_send_sem, meta_recv_sem, own_sem, load_sem,
):
    me = lax.axis_index("dev")
    cap, width = out.shape
    owned = cent.shape[0]
    entries = n * slots
    groups = entries // LANES
    per = LANES // slots
    wide = width // chunks

    load_cent = pltpu.make_async_copy(cent, cent_buf, load_sem.at[0])
    load_rot = pltpu.make_async_copy(rot, rot_buf, load_sem.at[1])
    own_meta = pltpu.make_async_copy(meta.at[me], meta_in.at[me], own_sem.at[chunks])

    def own_rows(c):
        cols = pl.ds(pl.multiple_of(c * wide, wide), wide)
        return pltpu.make_async_copy(send.at[me, :, cols], recv.at[c, me], own_sem.at[c])

    barrier = pltpu.get_barrier_semaphore()

    def greet(k, carry):
        peer = lax.rem(me + k, n)
        pl.semaphore_signal(barrier, inc=1, device_id=(peer,), device_id_type=MESH)
        return carry

    lax.fori_loop(1, n, greet, 0)
    own_meta.start()
    pl.semaphore_wait(barrier, n - 1)

    def peer_of(j):
        k = n // 2 + (2 * lax.rem(j, 2) - 1) * lax.div(j + 1, 2)
        return lax.rem(me + k, n)

    def send_meta(j, carry):
        peer = peer_of(j)
        pltpu.make_async_remote_copy(
            src_ref=meta.at[peer], dst_ref=meta_in.at[me],
            send_sem=meta_send_sem, recv_sem=meta_recv_sem,
            device_id=(peer,), device_id_type=MESH,
        ).start()
        return carry

    lax.fori_loop(0, n - 1, send_meta, 0)

    for c in range(chunks):
        def send_rows(j, carry):
            peer = peer_of(j)
            pltpu.make_async_remote_copy(
                src_ref=send.at[peer, :, pl.ds(c * wide, wide)], dst_ref=recv.at[c, me],
                send_sem=send_sem.at[c], recv_sem=recv_sem.at[c],
                device_id=(peer,), device_id_type=MESH,
            ).start()
            return carry

        lax.fori_loop(0, n - 1, send_rows, 0)

    load_cent.start()
    load_rot.start()
    for c in range(chunks):
        own_rows(c).start()

    most = pl.ds(0, n - 1)
    pltpu.make_async_copy(meta_in.at[most], meta_in.at[most], meta_recv_sem).wait()
    own_meta.wait()

    list_row, id_row, key_row, key_col, list_col, id_col = [], [], [], [], [], []
    lane = lax.broadcasted_iota(jnp.int32, (1, LANES), 1)
    for g in range(groups):
        got = jnp.sum(meta_in[pl.ds(g * per, per)], axis=0)
        found = got[0:1] - 1
        safe = jnp.where(found >= 0, found, owned)
        key = safe * entries + (g * LANES) + lane
        list_row.append(safe)
        id_row.append(got[1:2])
        key_row.append(key)
        key_col.append(jnp.transpose(jnp.broadcast_to(key, (LANES, LANES))))
        list_col.append(jnp.transpose(jnp.broadcast_to(safe, (LANES, LANES))))
        id_col.append(jnp.transpose(jnp.broadcast_to(got[1:2], (LANES, LANES))))

    slot_at = lax.broadcasted_iota(jnp.int32, (cap, LANES), 0)
    slot_list = jnp.zeros((cap, LANES), jnp.int32)
    pos_col = []
    for g in range(groups):
        rank = jnp.zeros((1, LANES), jnp.int32)
        for h in range(groups):
            less = (key_col[h] < key_row[g]).astype(jnp.int32)
            rank = rank + jnp.sum(less, axis=0, keepdims=True)
        rank = jnp.where(list_row[g] < owned, rank, cap + entries)
        hit = slot_at == rank
        place[:, pl.ds(g * LANES, LANES)] = hit.astype(F32).astype(BF16)
        slot_list = slot_list + jnp.where(hit, list_row[g] + 1, 0)
        pos_col.append(jnp.transpose(jnp.broadcast_to(rank, (LANES, LANES))))
    at_list = jnp.sum(slot_list, axis=1, keepdims=True) - 1

    for q in range(cap // LANES):
        total = jnp.zeros((1, LANES), jnp.int32)
        for g in range(groups):
            hit = pos_col[g] == lane + q * LANES
            total = total + jnp.sum(jnp.where(hit, id_col[g] + 1, 0), axis=0, keepdims=True)
        ids_out[pl.ds(q, 1), :] = total - 1
    for q in range(owned // LANES):
        total = jnp.zeros((1, LANES), jnp.int32)
        for g in range(groups):
            less = (list_col[g] < lane + q * LANES).astype(jnp.int32)
            total = total + jnp.sum(less, axis=0, keepdims=True)
        off_out[pl.ds(q, 1), :] = total

    res[...] = jnp.zeros_like(res)
    load_cent.wait()
    step = 256

    def centre(t, carry):
        base = pl.multiple_of(t * step, step)
        table = lax.broadcasted_iota(jnp.int32, (cap, step), 1) + base
        pick = (table == at_list).astype(F32).astype(BF16)
        for c in range(chunks):
            cols = pl.ds(c * wide, wide)
            hi, lo = split(cent_buf[pl.ds(base, step), cols])
            res[:, cols] -= dot(pick, hi) + dot(pick, lo)
        return carry

    lax.fori_loop(0, owned // step, centre, 0)

    load_rot.wait()

    def halve(t, carry):
        rows = pl.ds(pl.multiple_of(t * LANES, LANES), LANES)
        hi, lo = split(rot_buf[rows, :])
        rot_hi[rows, :] = hi
        rot_lo[rows, :] = lo
        return carry

    lax.fori_loop(0, width // LANES, halve, 0)
    out[...] = jnp.zeros_like(out)

    def turn(c, carry):
        pltpu.make_async_copy(recv.at[c, most], recv.at[c, most], recv_sem.at[c]).wait()
        own_rows(c).wait()
        cols = pl.ds(pl.multiple_of(c * wide, wide), wide)
        hi, lo = split(recv[c].reshape(entries, wide))
        spots = place[...]
        left = res[:, cols] + (dot(spots, hi) + dot(spots, lo))
        left_hi, left_lo = split(left)

        def tile(t, inner):
            at = pl.ds(pl.multiple_of(t * 256, 256), 256)
            r_hi = rot_hi[cols, at]
            r_lo = rot_lo[cols, at]
            out[:, at] += dot(left_hi, r_hi) + dot(left_lo, r_hi) + dot(left_hi, r_lo)
            return inner

        lax.fori_loop(0, width // 256, tile, 0)
        return carry

    lax.fori_loop(0, chunks, turn, 0)

    pltpu.make_async_copy(meta_in.at[most], meta_in.at[most], meta_send_sem).wait()
    for c in range(chunks):
        pltpu.make_async_copy(recv.at[c, most], recv.at[c, most], send_sem.at[c]).wait()


def full(embeddings, lists, row_ids, centroids, rotation):
    rows, width = embeddings.shape
    owned = centroids.shape[0]
    n = lax.axis_size("dev")
    cap = 2 * rows
    slots = max(8, cap // n)
    chunks = 4
    entries = n * slots
    me = lax.axis_index("dev")
    owner = lists // owned
    index = jnp.arange(rows, dtype=jnp.int32)
    earlier = index[None, :] < index[:, None]
    slot = jnp.sum((owner[None, :] == owner[:, None]) & earlier, axis=1).astype(jnp.int32)
    target = owner * slots + slot
    table = jnp.arange(entries, dtype=jnp.int32)
    match = target[None, :] == table[:, None]
    send = jnp.dot(match.astype(F32), embeddings, precision=lax.Precision.HIGH, preferred_element_type=F32)
    send = send.reshape(n, slots, width)
    per = LANES // slots
    own_lanes = (jnp.arange(LANES, dtype=jnp.int32) // slots) == lax.rem(me, per)

    def spread(values):
        picked = jnp.sum(jnp.where(match, values[None, :], 0), axis=1).astype(jnp.int32)
        return jnp.where(own_lanes[None, :], jnp.tile(picked.reshape(n, slots), (1, per)), 0)

    meta = jnp.zeros((n, 8, LANES), jnp.int32)
    meta = jnp.stack([spread(lists - owner * owned + 1), spread(row_ids)] + [jnp.zeros((n, LANES), jnp.int32)] * 6, axis=1)
    wide = width // chunks
    vmem = pl.BlockSpec(memory_space=pltpu.VMEM)
    hbm = pl.BlockSpec(memory_space=pltpu.HBM)
    packed, ids, offsets = pl.pallas_call(
        functools.partial(kernel, n, slots, chunks),
        out_shape=(
            jax.ShapeDtypeStruct((cap, width), F32),
            jax.ShapeDtypeStruct((cap // LANES, LANES), jnp.int32),
            jax.ShapeDtypeStruct((owned // LANES, LANES), jnp.int32),
        ),
        in_specs=[hbm, hbm, hbm, hbm],
        out_specs=(vmem, vmem, vmem),
        scratch_shapes=[
            pltpu.VMEM((chunks, n, slots, wide), F32),
            pltpu.VMEM((n, 8, LANES), jnp.int32),
            pltpu.VMEM((owned, width), F32),
            pltpu.VMEM((width, width), F32),
            pltpu.VMEM((width, width), BF16),
            pltpu.VMEM((width, width), BF16),
            pltpu.VMEM((cap, width), F32),
            pltpu.VMEM((cap, entries), BF16),
            pltpu.SemaphoreType.DMA((chunks,)),
            pltpu.SemaphoreType.DMA((chunks,)),
            pltpu.SemaphoreType.DMA,
            pltpu.SemaphoreType.DMA,
            pltpu.SemaphoreType.DMA((chunks + 1,)),
            pltpu.SemaphoreType.DMA((2,)),
        ],
        compiler_params=pltpu.CompilerParams(
            collective_id=1, has_side_effects=True, vmem_limit_bytes=48 * 1024 * 1024
        ),
    )(send, meta, centroids, rotation)
    return packed


def dot_t(a, b):
    return lax.dot_general(a, b, (((1,), (1,)), ((), ())), preferred_element_type=F32)


def hot(mask):
    return mask.astype(F32).astype(BF16)


def column_of(row):
    return jnp.transpose(jnp.broadcast_to(row, (LANES, LANES)))


def relayed_kernel(
    n, real, near, direct, pool,
    emb, lists, ids, cent, rot,
    out, ids_out, off_out, most_out,
    send_a, send_b, send_x, far_out, near_out, next_out, meta, recv, far_in, near_in, next_in, meta_in,
    part_1, part_2, part_3, cent_buf, rot_buf, rot_hi, rot_lo, res, left_hi, left_lo, place,
    send_sem, recv_sem, load_sem,
):
    me = lax.axis_index("dev")
    count, width = emb.shape
    cap = out.shape[0]
    owned = cent.shape[0]
    tall = width // LANES
    parts = count // LANES
    entries = n * real
    groups = entries // LANES
    members = n // LEVELS
    late = direct - near
    extra = real - direct
    block = far_in.shape[0]
    level = lax.div(me, members)
    inside = lax.rem(me, members)
    beside = level + 1 - 2 * lax.rem(level, 2)
    across = lax.rem(level + 2, LEVELS)
    corner = lax.rem(beside + 2, LEVELS)
    META, A, B, X, FAR, NEAR, NEXT = range(7)

    def flat(ref):
        return ref.reshape(ref.shape[0] * ref.shape[1] * tall, LANES) if len(ref.shape) == 4 else ref.reshape(ref.shape[0] * tall, LANES)

    recv_f, send_a_f, send_b_f, send_x_f = flat(recv), flat(send_a), flat(send_b), flat(send_x)
    far_out_f, near_out_f, next_out_f = flat(far_out), flat(near_out), flat(next_out)
    far_in_f, near_in_f, next_in_f = flat(far_in), flat(near_in), flat(next_in)
    part_1_f, part_2_f, part_3_f = flat(part_1), flat(part_2), flat(part_3)

    def tile_of(index):
        return pl.ds(pl.multiple_of(index * tall, 8), tall)

    load_cent = pltpu.make_async_copy(cent, cent_buf, load_sem.at[0])
    load_rot = pltpu.make_async_copy(rot, rot_buf, load_sem.at[1])
    barrier = pltpu.get_barrier_semaphore()

    def greet(k, carry):
        peer = lax.rem(me + k, n)
        pl.semaphore_signal(barrier, inc=1, device_id=(peer,), device_id_type=MESH)
        return carry

    lax.fori_loop(1, n, greet, 0)
    load_rot.start()
    load_cent.start()

    lane = lax.broadcasted_iota(jnp.int32, (1, LANES), 1)
    lanes = lax.broadcasted_iota(jnp.int32, (LANES, LANES), 1)
    subs = lax.broadcasted_iota(jnp.int32, (LANES, LANES), 0)
    ahead = subs < lanes

    list_of = [lists[r:r + 1, :] for r in range(parts)]
    id_of = [ids[r:r + 1, :] for r in range(parts)]
    owner_of = [lax.div(x, owned) for x in list_of]
    owner_col = [column_of(x) for x in owner_of]
    slot_of = []
    for r in range(parts):
        slot = jnp.zeros((1, LANES), jnp.int32)
        for q in range(r + 1):
            same = owner_col[q] == owner_of[r]
            if q == r:
                same = same & ahead
            slot = slot + jnp.sum(same.astype(jnp.int32), axis=0, keepdims=True)
        slot_of.append(slot)
    level_of = [lax.div(x, members) for x in owner_of]
    late_of = [slot_of[r] >= direct for r in range(parts)]
    home = [late_of[r] & (level_of[r] == level) for r in range(parts)]
    side = [late_of[r] & (level_of[r] == beside) for r in range(parts)]
    turn = [late_of[r] & (level_of[r] == corner) for r in range(parts)]
    gone = [late_of[r] & ((level_of[r] == across) | (level_of[r] == corner)) for r in range(parts)]
    seat = lax.broadcasted_iota(jnp.int32, (8, LANES), 0)
    triangle = hot(ahead)
    done = jnp.zeros((8, 1), F32)
    side_at, gone_at, turn_at = [], [], []
    for r in range(parts):
        mask = ((seat == 0) & side[r]) | ((seat == 1) & gone[r]) | ((seat == 2) & turn[r])
        flags = mask.astype(F32)
        index = (dot(flags.astype(BF16), triangle) + done).astype(jnp.int32)
        done = done + jnp.sum(flags, axis=1, keepdims=True)
        side_at.append(jnp.where(side[r], index[0:1], -1))
        gone_at.append(jnp.where(gone[r], index[1:2], -1))
        turn_at.append(jnp.where(turn[r], index[2:3], -1))
    worst = jnp.max(done, axis=0, keepdims=True).astype(jnp.int32)

    base_x = late * n
    base_far = base_x + extra * members
    base_near = base_far + block
    wanted = base_near + block
    table = lax.broadcasted_iota(jnp.int32, (wanted, LANES), 0)
    picks = []
    for r in range(parts):
        owner, slot = owner_of[r], slot_of[r]
        spot = (slot - direct) * members + lax.rem(owner, members)
        target = jnp.where((slot >= near) & (slot < direct), (slot - near) * n + owner, -1)
        target = jnp.where(home[r], base_x + spot, target)
        target = jnp.where((gone_at[r] >= 0) & (gone_at[r] < pool), base_far + gone_at[r], target)
        target = jnp.where((side_at[r] >= 0) & (side_at[r] < pool), base_near + side_at[r], target)
        picks.append(hot(table == target))
    pick = jnp.concatenate(picks, axis=1)
    for b in range(0, tall, 2):
        hi, lo = split(emb[:, b * LANES:(b + 2) * LANES])
        value = dot(pick, hi) + dot(pick, lo)
        for h in range(2):
            got = value[:, h * LANES:(h + 1) * LANES]
            send_a_f[pl.ds(b + h, late * n, stride=tall), :] = got[:base_x]
            send_x_f[pl.ds(b + h, extra * members, stride=tall), :] = got[base_x:base_far]
            far_out_f[pl.ds(b + h, block, stride=tall), :] = got[base_far:base_near]
            near_out_f[pl.ds(b + h, block, stride=tall), :] = got[base_near:]

    far_codes = jnp.zeros((8, LANES), F32)
    near_codes = jnp.zeros((8, LANES), F32)
    for r in range(parts):
        spot = (slot_of[r] - direct) * members + lax.rem(owner_of[r], members) + 1
        stay = gone[r] & (level_of[r] == across)
        first = jnp.where((seat == 0) & stay, spot, 0) + jnp.where((seat == 1) & turn[r], turn_at[r] + 1, 0)
        last = jnp.where(seat == 2, spot, 0)
        far_codes = far_codes + dot_t(first.astype(F32).astype(BF16), hot(subs == gone_at[r]))
        far_codes = far_codes + dot_t(last.astype(F32).astype(BF16), hot(subs == turn_at[r]))
        near_codes = near_codes + dot_t(last.astype(F32).astype(BF16), hot(subs == side_at[r]))
    far_out[pool] = far_codes - 1.0
    near_out[pool] = near_codes - 1.0
    blank = jnp.zeros((8, LANES), F32)
    for ref in (far_in, near_in, next_in):
        for k in range(pool + 1, block):
            ref[k] = blank

    owners = lax.broadcasted_iota(jnp.int32, (n, LANES), 0)
    high = jnp.zeros((n, LANES), F32)
    low = jnp.zeros((n, LANES), F32)
    for r in range(parts):
        mine = owners == owner_of[r]
        local = list_of[r] - owner_of[r] * owned + 1
        for values, shift in ((local, 0), (id_of[r], real)):
            spots = hot(subs == slot_of[r] + shift)
            upper = lax.div(values, 256)
            lower = values - upper * 256
            high = high + dot_t(jnp.where(mine, upper, 0).astype(F32).astype(BF16), spots)
            low = low + dot_t(jnp.where(mine, lower, 0).astype(F32).astype(BF16), spots)
    note = high.astype(jnp.int32) * 256 + low.astype(jnp.int32)
    meta[:, 0, :] = jnp.where(lane == 2 * real, worst, note)

    meta_in[pl.ds(me, 1)] = meta[pl.ds(me, 1)]
    for s in range(late):
        recv_f[tile_of((near + s) * n + me), :] = send_a_f[tile_of(s * n + me), :]
    for s in range(extra):
        recv_f[tile_of((direct + s) * n + me), :] = send_x_f[tile_of(s * members + inside), :]
    pl.semaphore_wait(barrier, n - 1)

    def post(src, dst, peer, at):
        pltpu.make_async_remote_copy(
            src_ref=src, dst_ref=dst, send_sem=send_sem.at[at], recv_sem=recv_sem.at[at],
            device_id=(peer,), device_id_type=MESH,
        ).start()

    def settle(ref, sem):
        pltpu.make_async_copy(ref, ref, sem).wait()

    def peer_of(k):
        peer, bit = 0, 1
        while bit < n:
            ours = lax.rem(lax.div(me, bit), 2)
            step = lax.rem(lax.div(k, bit), 2)
            peer = peer + bit * lax.rem(ours + step, 2)
            bit *= 2
        return peer

    def send_meta(k, carry):
        peer = peer_of(k)
        post(meta.at[peer], meta_in.at[me], peer, META)
        return carry

    def send_first(k, carry):
        peer = peer_of(k)
        post(send_a.at[:, peer], recv.at[pl.ds(near, late), me], peer, A)
        return carry

    def send_second(k, carry):
        peer = peer_of(k)
        post(send_b.at[:, peer], recv.at[pl.ds(0, near), me], peer, B)
        return carry

    def spread(ref, source):
        def one(k, carry):
            other = lax.rem(inside + k, members)
            post(ref.at[:, other], recv.at[pl.ds(direct, extra), source], level * members + other, X)
            return carry
        lax.fori_loop(1, members, one, 0)

    message = pl.ds(0, pool + 1)
    beside_dev = beside * members + inside
    across_dev = across * members + inside
    corner_dev = corner * members + inside

    lax.fori_loop(1, n, send_meta, 0)
    post(far_out.at[message], far_in.at[message], across_dev, FAR)
    post(near_out.at[message], near_in.at[message], beside_dev, NEAR)
    lax.fori_loop(1, n, send_first, 0)
    spread(send_x, me)

    span_meta = meta_in.at[pl.ds(0, n - 1)]
    settle(span_meta, recv_sem.at[META])

    got = meta_in[:, 0, :]
    if n < LANES:
        got = jnp.concatenate([got, jnp.zeros((LANES - n, LANES), jnp.int32)], axis=0)
    fields = jnp.transpose(got)
    most_out[...] = jnp.broadcast_to(jnp.max(fields[2 * real:2 * real + 1, :], axis=1, keepdims=True), (1, LANES))
    per = LANES // n
    rolled = [fields if k == 0 else pltpu.roll(fields, n * k, 1) for k in range(per)]

    def row_of(g, first):
        total = jnp.zeros((1, LANES), jnp.int32)
        for k in range(per):
            at = first + g * per + k
            total = total + rolled[k][at:at + 1, :]
        return total

    list_row, key_row, key_col, list_col, id_col = [], [], [], [], []
    for g in range(groups):
        found = row_of(g, 0) - 1
        safe = jnp.where(found >= 0, found, owned)
        entry = g * LANES + lane
        key = safe * entries + lax.rem(entry, n) * real + lax.div(entry, n)
        list_row.append(safe)
        key_row.append(key)
        key_col.append(column_of(key))
        list_col.append(column_of(safe))
        id_col.append(column_of(row_of(g, real)))

    slot_at = lax.broadcasted_iota(jnp.int32, (cap, LANES), 0)
    slot_list = jnp.zeros((cap, LANES), jnp.int32)
    pos_col = []
    for g in range(groups):
        rank = jnp.zeros((1, LANES), jnp.int32)
        for h in range(groups):
            less = (key_col[h] < key_row[g]).astype(jnp.int32)
            rank = rank + jnp.sum(less, axis=0, keepdims=True)
        rank = jnp.where(list_row[g] < owned, rank, cap + entries)
        hit = slot_at == rank
        place[:, pl.ds(g * LANES, LANES)] = hot(hit)
        slot_list = slot_list + jnp.where(hit, list_row[g] + 1, 0)
        pos_col.append(column_of(rank))
    at_list = jnp.sum(slot_list, axis=1, keepdims=True) - 1

    def piece(ref, first, rows, b):
        return ref[pl.ds(first * tall + b, rows, stride=tall), :]

    def pair(ref, first, rows, b):
        return split(jnp.concatenate([piece(ref, first, rows, b), piece(ref, first, rows, b + 1)], axis=1))

    seats = lax.broadcasted_iota(jnp.int32, (extra * members, block), 0)

    def expand(codes, source, target, forward):
        choose = hot(seats == codes[0][:, :block].astype(jnp.int32))
        if forward is not None:
            onward = lax.broadcasted_iota(jnp.int32, (block, block), 0) == codes[1][:, :block].astype(jnp.int32)
            choose = jnp.concatenate([choose, hot(onward)], axis=0)
        for b in range(0, tall, 2):
            hi, lo = pair(source, 0, block, b)
            value = dot(choose, hi) + dot(choose, lo)
            for h in range(2):
                part = value[:, h * LANES:(h + 1) * LANES]
                target[pl.ds(b + h, extra * members, stride=tall), :] = part[:extra * members]
                if forward is not None:
                    forward[pl.ds(b + h, block, stride=tall), :] = part[extra * members:]

    def keep(ref, source):
        for s in range(extra):
            recv_f[tile_of((direct + s) * n + source), :] = ref[tile_of(s * members + inside), :]

    settle(near_in.at[message], recv_sem.at[NEAR])
    expand([near_in[pool][2:3]], near_in_f, part_1_f, None)
    spread(part_1, beside_dev)
    keep(part_1_f, beside_dev)

    settle(far_in.at[message], recv_sem.at[FAR])
    codes = far_in[pool]
    expand([codes[0:1], codes[1:2]], far_in_f, part_2_f, next_out_f)
    next_out[pool] = codes
    post(next_out.at[message], next_in.at[message], beside_dev, NEXT)
    spread(part_2, across_dev)
    keep(part_2_f, across_dev)

    load_rot.wait()

    def halve(t, carry):
        at = pl.ds(pl.multiple_of(t * LANES, LANES), LANES)
        hi, lo = split(rot_buf[at, :])
        rot_hi[at, :] = hi
        rot_lo[at, :] = lo
        return carry

    lax.fori_loop(0, width // LANES, halve, 0)

    table = lax.broadcasted_iota(jnp.int32, (near * n, LANES), 0)
    pick = jnp.concatenate(
        [hot(table == jnp.where(slot_of[r] < near, slot_of[r] * n + owner_of[r], -1)) for r in range(parts)], axis=1
    )
    lines = pl.ds(0, near * n)
    for b in range(0, tall, 2):
        cols = pl.ds(b * LANES, 2 * LANES)
        hi, lo = split(emb[:, b * LANES:(b + 2) * LANES])
        hi, lo = split(dot(pick, hi) + dot(pick, lo))
        left_hi[lines, cols] = hi
        left_lo[lines, cols] = lo
    for b in range(0, tall, 2):
        at = pl.ds(b * LANES, 2 * LANES)
        r_hi = rot_hi[:, at]
        value = dot(left_hi[lines, :], r_hi) + dot(left_lo[lines, :], r_hi) + dot(left_hi[lines, :], rot_lo[:, at])
        for h in range(2):
            send_b_f[pl.ds(b + h, near * n, stride=tall), :] = value[:, h * LANES:(h + 1) * LANES]
    for s in range(near):
        recv_f[tile_of(s * n + me), :] = send_b_f[tile_of(s * n + me), :]
    lax.fori_loop(1, n, send_second, 0)

    for q in range(cap // LANES):
        total = jnp.zeros((1, LANES), jnp.int32)
        for g in range(groups):
            hit = pos_col[g] == lane + q * LANES
            total = total + jnp.sum(jnp.where(hit, id_col[g] + 1, 0), axis=0, keepdims=True)
        ids_out[pl.ds(q, 1), :] = total - 1
    for q in range(owned // LANES):
        total = jnp.zeros((1, LANES), jnp.int32)
        for g in range(groups):
            less = (list_col[g] < lane + q * LANES).astype(jnp.int32)
            total = total + jnp.sum(less, axis=0, keepdims=True)
        off_out[pl.ds(q, 1), :] = total

    settle(next_in.at[message], recv_sem.at[NEXT])
    expand([next_in[pool][2:3]], next_in_f, part_3_f, None)
    spread(part_3, corner_dev)
    keep(part_3_f, corner_dev)

    res[...] = jnp.zeros_like(res)
    load_cent.wait()
    step = 256

    def centre(t, carry):
        base = pl.multiple_of(t * step, step)
        table = lax.broadcasted_iota(jnp.int32, (cap, step), 1) + base
        pick = hot(table == at_list)
        for c in range(width // step):
            cols = pl.ds(c * step, step)
            hi, lo = split(cent_buf[pl.ds(base, step), cols])
            res[:, cols] -= dot(pick, hi) + dot(pick, lo)
        return carry

    lax.fori_loop(0, owned // step, centre, 0)

    span_a = recv.at[pl.ds(near, late), pl.ds(0, n - 1)]
    settle(span_a, recv_sem.at[A])
    span_x = recv_f.at[pl.ds(0, LEVELS * extra * (members - 1) * tall)]
    settle(span_x, recv_sem.at[X])
    rest = entries - near * n
    for b in range(0, tall, 2):
        cols = pl.ds(b * LANES, 2 * LANES)
        hi, lo = pair(recv_f, near * n, rest, b)
        spots = place[:, near * n:]
        hi, lo = split(res[:, cols] + dot(spots, hi) + dot(spots, lo))
        left_hi[:, cols] = hi
        left_lo[:, cols] = lo

    def tile(t, carry):
        at = pl.ds(pl.multiple_of(t * 256, 256), 256)
        r_hi = rot_hi[:, at]
        out[:, at] = dot(left_hi[...], r_hi) + dot(left_lo[...], r_hi) + dot(left_hi[...], rot_lo[:, at])
        return carry

    lax.fori_loop(0, width // 256, tile, 0)

    span_b = recv.at[pl.ds(0, near), pl.ds(0, n - 1)]
    settle(span_b, recv_sem.at[B])
    for b in range(0, tall, 2):
        cols = pl.ds(b * LANES, 2 * LANES)
        hi, lo = pair(recv_f, 0, near * n, b)
        spots = place[:, :near * n]
        out[:, cols] += dot(spots, hi) + dot(spots, lo)

    settle(span_meta, send_sem.at[META])
    settle(span_a, send_sem.at[A])
    settle(span_b, send_sem.at[B])
    settle(span_x, send_sem.at[X])
    settle(far_in.at[message], send_sem.at[FAR])
    settle(near_in.at[message], send_sem.at[NEAR])
    settle(next_in.at[message], send_sem.at[NEXT])


def emit_kernel(rows, ids, offsets, rows_out, ids_out, off_out, sem):
    moves = [
        pltpu.make_async_copy(src, dst, sem.at[k])
        for k, (src, dst) in enumerate(((rows, rows_out), (ids, ids_out), (offsets, off_out)))
    ]
    for move in moves:
        move.start()
    for move in moves:
        move.wait()


def emit(rows, ids, offsets):
    vmem = pl.BlockSpec(memory_space=pltpu.VMEM)
    hbm = pl.BlockSpec(memory_space=pltpu.HBM)
    return pl.pallas_call(
        emit_kernel,
        out_shape=tuple(jax.ShapeDtypeStruct(x.shape, x.dtype) for x in (rows, ids, offsets)),
        in_specs=[vmem] * 3,
        out_specs=(hbm,) * 3,
        scratch_shapes=[pltpu.SemaphoreType.DMA((3,))],
    )(rows, ids, offsets)


LEVELS = 4
POOL = 46


def local(embeddings, lists, row_ids, centroids, rotation):
    row_count, width = embeddings.shape
    owned = centroids.shape[0]
    n = lax.axis_size("dev")
    cap = 2 * row_count
    real = cap // n
    near = LANES // n
    direct = (7 * real + 8) // 16
    late, extra = direct - near, real - direct
    members = n // LEVELS
    pool = POOL
    block = -(-(pool + 1) // 16) * 16
    tall = width // LANES
    by_lane = (row_count // LANES, LANES)
    vmem = pl.BlockSpec(memory_space=pltpu.VMEM)
    hbm = pl.BlockSpec(memory_space=pltpu.HBM)

    def rows_of(*lead):
        return pltpu.VMEM((*lead, tall, LANES), F32)

    packed, ids, offsets, most = pl.pallas_call(
        functools.partial(relayed_kernel, n, real, near, direct, pool),
        out_shape=(
            jax.ShapeDtypeStruct((cap, width), F32),
            jax.ShapeDtypeStruct((cap // LANES, LANES), jnp.int32),
            jax.ShapeDtypeStruct((owned // LANES, LANES), jnp.int32),
            jax.ShapeDtypeStruct((1, LANES), jnp.int32),
        ),
        in_specs=[vmem] * 3 + [hbm] * 2,
        out_specs=(vmem,) * 4,
        scratch_shapes=[
            rows_of(late, n), rows_of(near, n), rows_of(extra, members), rows_of(block), rows_of(block), rows_of(block),
            pltpu.VMEM((n, 1, LANES), jnp.int32),
            rows_of(real, n), rows_of(block), rows_of(block), rows_of(block),
            pltpu.VMEM((n, 1, LANES), jnp.int32),
            rows_of(extra, members), rows_of(extra, members), rows_of(extra, members),
            pltpu.VMEM((owned, width), F32),
            pltpu.VMEM((width, width), F32),
            pltpu.VMEM((width, width), BF16),
            pltpu.VMEM((width, width), BF16),
            pltpu.VMEM((cap, width), F32),
            pltpu.VMEM((cap, width), BF16),
            pltpu.VMEM((cap, width), BF16),
            pltpu.VMEM((cap, n * real), BF16),
            pltpu.SemaphoreType.DMA((7,)),
            pltpu.SemaphoreType.DMA((7,)),
            pltpu.SemaphoreType.DMA((2,)),
        ],
        compiler_params=pltpu.CompilerParams(
            collective_id=0, has_side_effects=True, vmem_limit_bytes=48 * 1024 * 1024
        ),
    )(embeddings, lists.reshape(by_lane), row_ids.reshape(by_lane), centroids, rotation)
    packed, ids, offsets = lax.cond(
        most[0, 0] > pool,
        lambda: (full(embeddings, lists, row_ids, centroids, rotation), ids, offsets),
        lambda: emit(packed, ids, offsets),
    )
    return packed, ids.reshape(-1), offsets.reshape(-1)


def solution(mesh):
    in_specs = (P("dev", None), P("dev"), P("dev"), P("dev", None), P())
    out_specs = (P("dev", None), P("dev"), P("dev"))
    return jax.shard_map(local, mesh=mesh, in_specs=in_specs, out_specs=out_specs, check_vma=False)
```

```python
import functools

import jax
import jax.numpy as jnp
from jax import lax
from jax.experimental import pallas as pl
from jax.experimental.pallas import tpu as pltpu
from jax.sharding import PartitionSpec as P

MESH = pl.DeviceIdType.MESH
F32 = jnp.float32
BF16 = jnp.bfloat16
LANES = 128


def split(x):
    hi = x.astype(BF16)
    lo = (x - hi.astype(F32)).astype(BF16)
    return hi, lo


def dot(a, b):
    return jnp.dot(a, b, preferred_element_type=F32)


def kernel(
    n, slots, chunks,
    send, meta, cent, rot,
    out, ids_out, off_out,
    recv, meta_in, cent_buf, rot_buf, rot_hi, rot_lo, res, place,
    send_sem, recv_sem, meta_send_sem, meta_recv_sem, own_sem, load_sem,
):
    me = lax.axis_index("dev")
    cap, width = out.shape
    owned = cent.shape[0]
    entries = n * slots
    groups = entries // LANES
    per = LANES // slots
    wide = width // chunks

    load_cent = pltpu.make_async_copy(cent, cent_buf, load_sem.at[0])
    load_rot = pltpu.make_async_copy(rot, rot_buf, load_sem.at[1])
    own_meta = pltpu.make_async_copy(meta.at[me], meta_in.at[me], own_sem.at[chunks])

    def own_rows(c):
        cols = pl.ds(pl.multiple_of(c * wide, wide), wide)
        return pltpu.make_async_copy(send.at[me, :, cols], recv.at[c, me], own_sem.at[c])

    barrier = pltpu.get_barrier_semaphore()

    def greet(k, carry):
        peer = lax.rem(me + k, n)
        pl.semaphore_signal(barrier, inc=1, device_id=(peer,), device_id_type=MESH)
        return carry

    lax.fori_loop(1, n, greet, 0)
    own_meta.start()
    pl.semaphore_wait(barrier, n - 1)

    def peer_of(j):
        k = n // 2 + (2 * lax.rem(j, 2) - 1) * lax.div(j + 1, 2)
        return lax.rem(me + k, n)

    def send_meta(j, carry):
        peer = peer_of(j)
        pltpu.make_async_remote_copy(
            src_ref=meta.at[peer], dst_ref=meta_in.at[me],
            send_sem=meta_send_sem, recv_sem=meta_recv_sem,
            device_id=(peer,), device_id_type=MESH,
        ).start()
        return carry

    lax.fori_loop(0, n - 1, send_meta, 0)

    for c in range(chunks):
        def send_rows(j, carry):
            peer = peer_of(j)
            pltpu.make_async_remote_copy(
                src_ref=send.at[peer, :, pl.ds(c * wide, wide)], dst_ref=recv.at[c, me],
                send_sem=send_sem.at[c], recv_sem=recv_sem.at[c],
                device_id=(peer,), device_id_type=MESH,
            ).start()
            return carry

        lax.fori_loop(0, n - 1, send_rows, 0)

    load_cent.start()
    load_rot.start()
    for c in range(chunks):
        own_rows(c).start()

    most = pl.ds(0, n - 1)
    pltpu.make_async_copy(meta_in.at[most], meta_in.at[most], meta_recv_sem).wait()
    own_meta.wait()

    list_row, id_row, key_row, key_col, list_col, id_col = [], [], [], [], [], []
    lane = lax.broadcasted_iota(jnp.int32, (1, LANES), 1)
    for g in range(groups):
        got = jnp.sum(meta_in[pl.ds(g * per, per)], axis=0)
        found = got[0:1] - 1
        safe = jnp.where(found >= 0, found, owned)
        key = safe * entries + (g * LANES) + lane
        list_row.append(safe)
        id_row.append(got[1:2])
        key_row.append(key)
        key_col.append(jnp.transpose(jnp.broadcast_to(key, (LANES, LANES))))
        list_col.append(jnp.transpose(jnp.broadcast_to(safe, (LANES, LANES))))
        id_col.append(jnp.transpose(jnp.broadcast_to(got[1:2], (LANES, LANES))))

    slot_at = lax.broadcasted_iota(jnp.int32, (cap, LANES), 0)
    slot_list = jnp.zeros((cap, LANES), jnp.int32)
    pos_col = []
    for g in range(groups):
        rank = jnp.zeros((1, LANES), jnp.int32)
        for h in range(groups):
            less = (key_col[h] < key_row[g]).astype(jnp.int32)
            rank = rank + jnp.sum(less, axis=0, keepdims=True)
        rank = jnp.where(list_row[g] < owned, rank, cap + entries)
        hit = slot_at == rank
        place[:, pl.ds(g * LANES, LANES)] = hit.astype(F32).astype(BF16)
        slot_list = slot_list + jnp.where(hit, list_row[g] + 1, 0)
        pos_col.append(jnp.transpose(jnp.broadcast_to(rank, (LANES, LANES))))
    at_list = jnp.sum(slot_list, axis=1, keepdims=True) - 1

    for q in range(cap // LANES):
        total = jnp.zeros((1, LANES), jnp.int32)
        for g in range(groups):
            hit = pos_col[g] == lane + q * LANES
            total = total + jnp.sum(jnp.where(hit, id_col[g] + 1, 0), axis=0, keepdims=True)
        ids_out[pl.ds(q, 1), :] = total - 1
    for q in range(owned // LANES):
        total = jnp.zeros((1, LANES), jnp.int32)
        for g in range(groups):
            less = (list_col[g] < lane + q * LANES).astype(jnp.int32)
            total = total + jnp.sum(less, axis=0, keepdims=True)
        off_out[pl.ds(q, 1), :] = total

    res[...] = jnp.zeros_like(res)
    load_cent.wait()
    step = 256

    def centre(t, carry):
        base = pl.multiple_of(t * step, step)
        table = lax.broadcasted_iota(jnp.int32, (cap, step), 1) + base
        pick = (table == at_list).astype(F32).astype(BF16)
        for c in range(chunks):
            cols = pl.ds(c * wide, wide)
            hi, lo = split(cent_buf[pl.ds(base, step), cols])
            res[:, cols] -= dot(pick, hi) + dot(pick, lo)
        return carry

    lax.fori_loop(0, owned // step, centre, 0)

    load_rot.wait()

    def halve(t, carry):
        rows = pl.ds(pl.multiple_of(t * LANES, LANES), LANES)
        hi, lo = split(rot_buf[rows, :])
        rot_hi[rows, :] = hi
        rot_lo[rows, :] = lo
        return carry

    lax.fori_loop(0, width // LANES, halve, 0)
    out[...] = jnp.zeros_like(out)

    def turn(c, carry):
        pltpu.make_async_copy(recv.at[c, most], recv.at[c, most], recv_sem.at[c]).wait()
        own_rows(c).wait()
        cols = pl.ds(pl.multiple_of(c * wide, wide), wide)
        hi, lo = split(recv[c].reshape(entries, wide))
        spots = place[...]
        left = res[:, cols] + (dot(spots, hi) + dot(spots, lo))
        left_hi, left_lo = split(left)

        def tile(t, inner):
            at = pl.ds(pl.multiple_of(t * 256, 256), 256)
            r_hi = rot_hi[cols, at]
            r_lo = rot_lo[cols, at]
            out[:, at] += dot(left_hi, r_hi) + dot(left_lo, r_hi) + dot(left_hi, r_lo)
            return inner

        lax.fori_loop(0, width // 256, tile, 0)
        return carry

    lax.fori_loop(0, chunks, turn, 0)

    pltpu.make_async_copy(meta_in.at[most], meta_in.at[most], meta_send_sem).wait()
    for c in range(chunks):
        pltpu.make_async_copy(recv.at[c, most], recv.at[c, most], send_sem.at[c]).wait()


def full(embeddings, lists, row_ids, centroids, rotation):
    rows, width = embeddings.shape
    owned = centroids.shape[0]
    n = lax.axis_size("dev")
    cap = 2 * rows
    slots = max(8, cap // n)
    chunks = 4
    entries = n * slots
    me = lax.axis_index("dev")
    owner = lists // owned
    index = jnp.arange(rows, dtype=jnp.int32)
    earlier = index[None, :] < index[:, None]
    slot = jnp.sum((owner[None, :] == owner[:, None]) & earlier, axis=1).astype(jnp.int32)
    target = owner * slots + slot
    table = jnp.arange(entries, dtype=jnp.int32)
    match = target[None, :] == table[:, None]
    send = jnp.dot(match.astype(F32), embeddings, precision=lax.Precision.HIGH, preferred_element_type=F32)
    send = send.reshape(n, slots, width)
    per = LANES // slots
    own_lanes = (jnp.arange(LANES, dtype=jnp.int32) // slots) == lax.rem(me, per)

    def spread(values):
        picked = jnp.sum(jnp.where(match, values[None, :], 0), axis=1).astype(jnp.int32)
        return jnp.where(own_lanes[None, :], jnp.tile(picked.reshape(n, slots), (1, per)), 0)

    meta = jnp.zeros((n, 8, LANES), jnp.int32)
    meta = jnp.stack([spread(lists - owner * owned + 1), spread(row_ids)] + [jnp.zeros((n, LANES), jnp.int32)] * 6, axis=1)
    wide = width // chunks
    vmem = pl.BlockSpec(memory_space=pltpu.VMEM)
    hbm = pl.BlockSpec(memory_space=pltpu.HBM)
    packed, ids, offsets = pl.pallas_call(
        functools.partial(kernel, n, slots, chunks),
        out_shape=(
            jax.ShapeDtypeStruct((cap, width), F32),
            jax.ShapeDtypeStruct((cap // LANES, LANES), jnp.int32),
            jax.ShapeDtypeStruct((owned // LANES, LANES), jnp.int32),
        ),
        in_specs=[hbm, hbm, hbm, hbm],
        out_specs=(vmem, vmem, vmem),
        scratch_shapes=[
            pltpu.VMEM((chunks, n, slots, wide), F32),
            pltpu.VMEM((n, 8, LANES), jnp.int32),
            pltpu.VMEM((owned, width), F32),
            pltpu.VMEM((width, width), F32),
            pltpu.VMEM((width, width), BF16),
            pltpu.VMEM((width, width), BF16),
            pltpu.VMEM((cap, width), F32),
            pltpu.VMEM((cap, entries), BF16),
            pltpu.SemaphoreType.DMA((chunks,)),
            pltpu.SemaphoreType.DMA((chunks,)),
            pltpu.SemaphoreType.DMA,
            pltpu.SemaphoreType.DMA,
            pltpu.SemaphoreType.DMA((chunks + 1,)),
            pltpu.SemaphoreType.DMA((2,)),
        ],
        compiler_params=pltpu.CompilerParams(
            collective_id=1, has_side_effects=True, vmem_limit_bytes=48 * 1024 * 1024
        ),
    )(send, meta, centroids, rotation)
    return packed


def dot_t(a, b):
    return lax.dot_general(a, b, (((1,), (1,)), ((), ())), preferred_element_type=F32)


def hot(mask):
    return mask.astype(F32).astype(BF16)


def column_of(row):
    return jnp.transpose(jnp.broadcast_to(row, (LANES, LANES)))


def relayed_kernel(
    n, real, near, direct, pool,
    emb_hbm, lists_hbm, ids_hbm, cent, rot,
    out, last_hi, last_lo, last_place, ids_out, off_out, most_out,
    emb, lists, ids, turned_hi, turned_lo, send_a, send_b, send_x, far_out, near_out, next_out, meta, recv, far_in, near_in, next_in, meta_in,
    part_1, part_2, part_3, cent_buf, rot_buf, rot_hi, rot_lo, res, left_hi, left_lo, place,
    send_sem, recv_sem, load_sem,
):
    me = lax.axis_index("dev")
    count, width = emb.shape
    cap = out.shape[0]
    owned = cent.shape[0]
    tall = width // LANES
    parts = count // LANES
    entries = n * real
    groups = entries // LANES
    members = n // LEVELS
    late = direct - near
    extra = real - direct
    block = far_in.shape[0]
    level = lax.div(me, members)
    inside = lax.rem(me, members)
    beside = level + 1 - 2 * lax.rem(level, 2)
    across = lax.rem(level + 2, LEVELS)
    corner = lax.rem(beside + 2, LEVELS)
    META, A, B, X, FAR, NEAR, NEXT = range(7)

    def flat(ref):
        return ref.reshape(ref.shape[0] * ref.shape[1] * tall, LANES) if len(ref.shape) == 4 else ref.reshape(ref.shape[0] * tall, LANES)

    recv_f, send_a_f, send_b_f, send_x_f = flat(recv), flat(send_a), flat(send_b), flat(send_x)
    far_out_f, near_out_f, next_out_f = flat(far_out), flat(near_out), flat(next_out)
    far_in_f, near_in_f, next_in_f = flat(far_in), flat(near_in), flat(next_in)
    part_1_f, part_2_f, part_3_f = flat(part_1), flat(part_2), flat(part_3)

    def tile_of(index):
        return pl.ds(pl.multiple_of(index * tall, 8), tall)

    load_cent = pltpu.make_async_copy(cent, cent_buf, load_sem.at[0])
    load_rot = pltpu.make_async_copy(rot, rot_buf, load_sem.at[1])
    barrier = pltpu.get_barrier_semaphore()

    def greet(k, carry):
        peer = lax.rem(me + k, n)
        pl.semaphore_signal(barrier, inc=1, device_id=(peer,), device_id_type=MESH)
        return carry

    lax.fori_loop(1, n, greet, 0)
    loads = [
        pltpu.make_async_copy(src, dst, load_sem.at[2 + k])
        for k, (src, dst) in enumerate(((lists_hbm, lists), (ids_hbm, ids), (emb_hbm, emb)))
    ]
    for load in loads:
        load.start()
    load_rot.start()
    for load in loads:
        load.wait()

    lane = lax.broadcasted_iota(jnp.int32, (1, LANES), 1)
    lanes = lax.broadcasted_iota(jnp.int32, (LANES, LANES), 1)
    subs = lax.broadcasted_iota(jnp.int32, (LANES, LANES), 0)
    ahead = subs < lanes

    list_of = [lists[r:r + 1, :] for r in range(parts)]
    id_of = [ids[r:r + 1, :] for r in range(parts)]
    owner_of = [lax.div(x, owned) for x in list_of]
    owner_col = [column_of(x) for x in owner_of]
    slot_of = []
    for r in range(parts):
        slot = jnp.zeros((1, LANES), jnp.int32)
        for q in range(r + 1):
            same = owner_col[q] == owner_of[r]
            if q == r:
                same = same & ahead
            slot = slot + jnp.sum(same.astype(jnp.int32), axis=0, keepdims=True)
        slot_of.append(slot)
    level_of = [lax.div(x, members) for x in owner_of]
    late_of = [slot_of[r] >= direct for r in range(parts)]
    home = [late_of[r] & (level_of[r] == level) for r in range(parts)]
    side = [late_of[r] & (level_of[r] == beside) for r in range(parts)]
    turn = [late_of[r] & (level_of[r] == corner) for r in range(parts)]
    gone = [late_of[r] & ((level_of[r] == across) | (level_of[r] == corner)) for r in range(parts)]
    seat = lax.broadcasted_iota(jnp.int32, (8, LANES), 0)
    triangle = hot(ahead)
    done = jnp.zeros((8, 1), F32)
    side_at, gone_at, turn_at = [], [], []
    for r in range(parts):
        mask = ((seat == 0) & side[r]) | ((seat == 1) & gone[r]) | ((seat == 2) & turn[r])
        flags = mask.astype(F32)
        index = (dot(flags.astype(BF16), triangle) + done).astype(jnp.int32)
        done = done + jnp.sum(flags, axis=1, keepdims=True)
        side_at.append(jnp.where(side[r], index[0:1], -1))
        gone_at.append(jnp.where(gone[r], index[1:2], -1))
        turn_at.append(jnp.where(turn[r], index[2:3], -1))
    worst = jnp.max(done, axis=0, keepdims=True).astype(jnp.int32)

    table = lax.broadcasted_iota(jnp.int32, (2 * block, LANES), 0)
    picks = []
    for r in range(parts):
        target = jnp.where((gone_at[r] >= 0) & (gone_at[r] < pool), gone_at[r], -1)
        target = jnp.where((side_at[r] >= 0) & (side_at[r] < pool), block + side_at[r], target)
        picks.append(hot(table == target))
    pick = jnp.concatenate(picks, axis=1)
    for b in range(0, tall, 2):
        hi, lo = split(emb[:, b * LANES:(b + 2) * LANES])
        left_hi[pl.ds(0, count), pl.ds(b * LANES, 2 * LANES)] = hi
        left_lo[pl.ds(0, count), pl.ds(b * LANES, 2 * LANES)] = lo
        value = dot(pick, hi) + dot(pick, lo)
        for h in range(2):
            got = value[:, h * LANES:(h + 1) * LANES]
            far_out_f[pl.ds(b + h, block, stride=tall), :] = got[:block]
            near_out_f[pl.ds(b + h, block, stride=tall), :] = got[block:]

    far_codes = jnp.zeros((8, LANES), F32)
    near_codes = jnp.zeros((8, LANES), F32)
    for r in range(parts):
        spot = (slot_of[r] - direct) * members + lax.rem(owner_of[r], members) + 1
        stay = gone[r] & (level_of[r] == across)
        first = jnp.where((seat == 0) & stay, spot, 0) + jnp.where((seat == 1) & turn[r], turn_at[r] + 1, 0)
        last = jnp.where(seat == 2, spot, 0)
        far_codes = far_codes + dot_t(first.astype(F32).astype(BF16), hot(subs == gone_at[r]))
        far_codes = far_codes + dot_t(last.astype(F32).astype(BF16), hot(subs == turn_at[r]))
        near_codes = near_codes + dot_t(last.astype(F32).astype(BF16), hot(subs == side_at[r]))
    far_out[pool] = far_codes - 1.0
    near_out[pool] = near_codes - 1.0
    blank = jnp.zeros((8, LANES), F32)
    for ref in (far_in, near_in, next_in):
        for k in range(pool + 1, block):
            ref[k] = blank

    owners = lax.broadcasted_iota(jnp.int32, (n, LANES), 0)
    high = jnp.zeros((n, LANES), F32)
    low = jnp.zeros((n, LANES), F32)
    for r in range(parts):
        mine = owners == owner_of[r]
        local = list_of[r] - owner_of[r] * owned + 1
        for values, shift in ((local, 0), (id_of[r], real)):
            spots = hot(subs == slot_of[r] + shift)
            upper = lax.div(values, 256)
            lower = values - upper * 256
            high = high + dot_t(jnp.where(mine, upper, 0).astype(F32).astype(BF16), spots)
            low = low + dot_t(jnp.where(mine, lower, 0).astype(F32).astype(BF16), spots)
    note = high.astype(jnp.int32) * 256 + low.astype(jnp.int32)
    meta[:, 0, :] = jnp.where(lane == 2 * real, worst, note)

    meta_in[pl.ds(me, 1)] = meta[pl.ds(me, 1)]
    pl.semaphore_wait(barrier, n - 1)

    def post(src, dst, peer, at):
        pltpu.make_async_remote_copy(
            src_ref=src, dst_ref=dst, send_sem=send_sem.at[at], recv_sem=recv_sem.at[at],
            device_id=(peer,), device_id_type=MESH,
        ).start()

    def settle(ref, sem):
        pltpu.make_async_copy(ref, ref, sem).wait()

    def peer_of(k):
        peer, bit = 0, 1
        while bit < n:
            ours = lax.rem(lax.div(me, bit), 2)
            step = lax.rem(lax.div(k, bit), 2)
            peer = peer + bit * lax.rem(ours + step, 2)
            bit *= 2
        return peer

    def send_meta(k, carry):
        peer = peer_of(k)
        post(meta.at[peer], meta_in.at[me], peer, META)
        return carry

    def send_first(k, carry):
        peer = peer_of(k)
        post(send_a.at[:, peer], recv.at[pl.ds(near, late), me], peer, A)
        return carry

    def send_second(k, carry):
        peer = peer_of(k)
        post(send_b.at[:, peer], recv.at[pl.ds(0, near), me], peer, B)
        return carry

    def spread(ref, source):
        def one(k, carry):
            other = lax.rem(inside + k, members)
            post(ref.at[:, other], recv.at[pl.ds(direct, extra), source], level * members + other, X)
            return carry
        lax.fori_loop(1, members, one, 0)

    message = pl.ds(0, pool + 1)
    beside_dev = beside * members + inside
    across_dev = across * members + inside
    corner_dev = corner * members + inside

    lax.fori_loop(1, n, send_meta, 0)
    post(far_out.at[message], far_in.at[message], across_dev, FAR)
    post(near_out.at[message], near_in.at[message], beside_dev, NEAR)
    load_rot.wait()
    load_cent.start()

    def halve(t, carry):
        at = pl.ds(pl.multiple_of(t * LANES, LANES), LANES)
        hi, lo = split(rot_buf[at, :])
        rot_hi[at, :] = hi
        rot_lo[at, :] = lo
        return carry

    lax.fori_loop(0, width // LANES, halve, 0)

    def turn_rows(lines):
        def turned(t, carry):
            at = pl.ds(pl.multiple_of(t * 256, 256), 256)
            r_hi = rot_hi[:, at]
            value = dot(left_hi[lines, :], r_hi) + dot(left_lo[lines, :], r_hi) + dot(left_hi[lines, :], rot_lo[:, at])
            hi, lo = split(value)
            turned_hi[lines, at] = hi
            turned_lo[lines, at] = lo
            return carry

        lax.fori_loop(0, width // 256, turned, 0)

    turn_rows(pl.ds(0, count))
    base_x = late * n
    base_b = base_x + extra * members
    wanted = base_b + near * n
    table = lax.broadcasted_iota(jnp.int32, (wanted, LANES), 0)
    picks = []
    for r in range(parts):
        owner, slot = owner_of[r], slot_of[r]
        spot = (slot - direct) * members + lax.rem(owner, members)
        target = jnp.where(slot < direct, (slot - near) * n + owner, -1)
        target = jnp.where(slot < near, base_b + slot * n + owner, target)
        target = jnp.where(home[r], base_x + spot, target)
        picks.append(hot(table == target))
    pick = jnp.concatenate(picks, axis=1)
    for b in range(0, tall, 2):
        cols = pl.ds(b * LANES, 2 * LANES)
        value = dot(pick, turned_hi[:, cols]) + dot(pick, turned_lo[:, cols])
        for h in range(2):
            got = value[:, h * LANES:(h + 1) * LANES]
            send_a_f[pl.ds(b + h, late * n, stride=tall), :] = got[:base_x]
            send_x_f[pl.ds(b + h, extra * members, stride=tall), :] = got[base_x:base_b]
            send_b_f[pl.ds(b + h, near * n, stride=tall), :] = got[base_b:]
    lax.fori_loop(1, n, send_first, 0)
    spread(send_x, me)
    for s in range(late):
        recv_f[tile_of((near + s) * n + me), :] = send_a_f[tile_of(s * n + me), :]
    for s in range(near):
        recv_f[tile_of(s * n + me), :] = send_b_f[tile_of(s * n + me), :]
    for s in range(extra):
        recv_f[tile_of((direct + s) * n + me), :] = send_x_f[tile_of(s * members + inside), :]

    span_meta = meta_in.at[pl.ds(0, n - 1)]
    settle(span_meta, recv_sem.at[META])

    got = meta_in[:, 0, :]
    if n < LANES:
        got = jnp.concatenate([got, jnp.zeros((LANES - n, LANES), jnp.int32)], axis=0)
    fields = jnp.transpose(got)
    most_out[...] = jnp.broadcast_to(jnp.max(fields[2 * real:2 * real + 1, :], axis=1, keepdims=True), (1, LANES))
    per = LANES // n
    rolled = [fields if k == 0 else pltpu.roll(fields, n * k, 1) for k in range(per)]

    def row_of(g, first):
        total = jnp.zeros((1, LANES), jnp.int32)
        for k in range(per):
            at = first + g * per + k
            total = total + rolled[k][at:at + 1, :]
        return total

    list_row, key_row, key_col, list_col, id_col = [], [], [], [], []
    for g in range(groups):
        found = row_of(g, 0) - 1
        safe = jnp.where(found >= 0, found, owned)
        entry = g * LANES + lane
        key = safe * entries + lax.rem(entry, n) * real + lax.div(entry, n)
        list_row.append(safe)
        key_row.append(key)
        key_col.append(column_of(key))
        list_col.append(column_of(safe))
        id_col.append(column_of(row_of(g, real)))

    slot_at = lax.broadcasted_iota(jnp.int32, (cap, LANES), 0)
    slot_list = jnp.zeros((cap, LANES), jnp.int32)
    pos_col = []
    for g in range(groups):
        rank = jnp.zeros((1, LANES), jnp.int32)
        for h in range(groups):
            less = (key_col[h] < key_row[g]).astype(jnp.int32)
            rank = rank + jnp.sum(less, axis=0, keepdims=True)
        rank = jnp.where(list_row[g] < owned, rank, cap + entries)
        hit = slot_at == rank
        place[:, pl.ds(g * LANES, LANES)] = hot(hit)
        slot_list = slot_list + jnp.where(hit, list_row[g] + 1, 0)
        pos_col.append(column_of(rank))
    at_list = jnp.sum(slot_list, axis=1, keepdims=True) - 1

    def piece(ref, first, rows, b):
        return ref[pl.ds(first * tall + b, rows, stride=tall), :]

    def pair(ref, first, rows, b):
        return split(jnp.concatenate([piece(ref, first, rows, b), piece(ref, first, rows, b + 1)], axis=1))

    seats = lax.broadcasted_iota(jnp.int32, (extra * members, block), 0)

    def expand(codes, source, target, forward, raw):
        choose = hot(seats == codes[0][:, :block].astype(jnp.int32))
        if forward is not None:
            onward = lax.broadcasted_iota(jnp.int32, (block, block), 0) == codes[1][:, :block].astype(jnp.int32)
            choose = jnp.concatenate([choose, hot(onward)], axis=0)
        lines = pl.ds(0, block)
        if raw:
            for b in range(0, tall, 2):
                cols = pl.ds(b * LANES, 2 * LANES)
                hi, lo = pair(source, 0, block, b)
                left_hi[lines, cols] = hi
                left_lo[lines, cols] = lo
            turn_rows(lines)
        for b in range(0, tall, 2):
            if raw:
                cols = pl.ds(b * LANES, 2 * LANES)
                hi, lo = turned_hi[lines, cols], turned_lo[lines, cols]
            else:
                hi, lo = pair(source, 0, block, b)
            value = dot(choose, hi) + dot(choose, lo)
            for h in range(2):
                part = value[:, h * LANES:(h + 1) * LANES]
                target[pl.ds(b + h, extra * members, stride=tall), :] = part[:extra * members]
                if forward is not None:
                    forward[pl.ds(b + h, block, stride=tall), :] = part[extra * members:]

    def keep(ref, source):
        for s in range(extra):
            recv_f[tile_of((direct + s) * n + source), :] = ref[tile_of(s * members + inside), :]

    settle(near_in.at[message], recv_sem.at[NEAR])
    expand([near_in[pool][2:3]], near_in_f, part_1_f, None, True)
    spread(part_1, beside_dev)
    keep(part_1_f, beside_dev)

    settle(far_in.at[message], recv_sem.at[FAR])
    codes = far_in[pool]
    expand([codes[0:1], codes[1:2]], far_in_f, part_2_f, next_out_f, True)
    next_out[pool] = codes
    post(next_out.at[message], next_in.at[message], beside_dev, NEXT)
    spread(part_2, across_dev)
    keep(part_2_f, across_dev)

    lax.fori_loop(1, n, send_second, 0)

    for q in range(cap // LANES):
        total = jnp.zeros((1, LANES), jnp.int32)
        for g in range(groups):
            hit = pos_col[g] == lane + q * LANES
            total = total + jnp.sum(jnp.where(hit, id_col[g] + 1, 0), axis=0, keepdims=True)
        ids_out[pl.ds(q, 1), :] = total - 1
    for q in range(owned // LANES):
        total = jnp.zeros((1, LANES), jnp.int32)
        for g in range(groups):
            less = (list_col[g] < lane + q * LANES).astype(jnp.int32)
            total = total + jnp.sum(less, axis=0, keepdims=True)
        off_out[pl.ds(q, 1), :] = total

    res[...] = jnp.zeros_like(res)
    load_cent.wait()
    step = 256

    def centre(t, carry):
        base = pl.multiple_of(t * step, step)
        table = lax.broadcasted_iota(jnp.int32, (cap, step), 1) + base
        pick = hot(table == at_list)
        for c in range(width // step):
            cols = pl.ds(c * step, step)
            hi, lo = split(cent_buf[pl.ds(base, step), cols])
            res[:, cols] -= dot(pick, hi) + dot(pick, lo)
        return carry

    lax.fori_loop(0, owned // step, centre, 0)

    settle(next_in.at[message], recv_sem.at[NEXT])
    expand([next_in[pool][2:3]], next_in_f, part_3_f, None, False)
    spread(part_3, corner_dev)
    keep(part_3_f, corner_dev)

    for b in range(0, tall, 2):
        cols = pl.ds(b * LANES, 2 * LANES)
        hi, lo = split(res[:, cols])
        left_hi[:, cols] = hi
        left_lo[:, cols] = lo

    def tile(t, carry):
        at = pl.ds(pl.multiple_of(t * 256, 256), 256)
        r_hi = rot_hi[:, at]
        out[:, at] = dot(left_hi[...], r_hi) + dot(left_lo[...], r_hi) + dot(left_hi[...], rot_lo[:, at])
        return carry

    lax.fori_loop(0, width // 256, tile, 0)

    span_a = recv.at[pl.ds(near, late), pl.ds(0, n - 1)]
    settle(span_a, recv_sem.at[A])
    span_x = recv_f.at[pl.ds(0, LEVELS * extra * (members - 1) * tall)]
    settle(span_x, recv_sem.at[X])
    rest = entries - near * n
    for b in range(0, tall, 2):
        cols = pl.ds(b * LANES, 2 * LANES)
        hi, lo = pair(recv_f, near * n, rest, b)
        spots = place[:, near * n:]
        out[:, cols] += dot(spots, hi) + dot(spots, lo)

    span_b = recv.at[pl.ds(0, near), pl.ds(0, n - 1)]
    settle(span_b, recv_sem.at[B])
    for b in range(0, tall, 2):
        cols = pl.ds(b * LANES, 2 * LANES)
        hi, lo = pair(recv_f, 0, near * n, b)
        last_hi[:, cols] = hi
        last_lo[:, cols] = lo
    last_place[...] = place[:, :near * n]

    settle(span_meta, send_sem.at[META])
    settle(span_a, send_sem.at[A])
    settle(span_b, send_sem.at[B])
    settle(span_x, send_sem.at[X])
    settle(far_in.at[message], send_sem.at[FAR])
    settle(near_in.at[message], send_sem.at[NEAR])
    settle(next_in.at[message], send_sem.at[NEXT])


def finish_kernel(rows, hi, lo, place, ids, offsets, rows_out, ids_out, off_out, buf, sem):
    wide = 256
    tiles = rows.shape[1] // wide
    moves = [
        pltpu.make_async_copy(ids, ids_out, sem.at[tiles]),
        pltpu.make_async_copy(offsets, off_out, sem.at[tiles + 1]),
    ]
    for move in moves:
        move.start()
    for t in range(tiles):
        cols = pl.ds(t * wide, wide)
        buf[t] = rows[:, cols] + dot(place[...], hi[:, cols]) + dot(place[...], lo[:, cols])
        move = pltpu.make_async_copy(buf.at[t], rows_out.at[:, cols], sem.at[t])
        move.start()
        moves.append(move)
    for move in moves:
        move.wait()


def finish(rows, hi, lo, place, ids, offsets):
    vmem = pl.BlockSpec(memory_space=pltpu.VMEM)
    hbm = pl.BlockSpec(memory_space=pltpu.HBM)
    cap, width = rows.shape
    return pl.pallas_call(
        finish_kernel,
        out_shape=tuple(jax.ShapeDtypeStruct(x.shape, x.dtype) for x in (rows, ids, offsets)),
        in_specs=[vmem] * 6,
        out_specs=(hbm,) * 3,
        scratch_shapes=[pltpu.VMEM((width // 256, cap, 256), F32), pltpu.SemaphoreType.DMA((width // 256 + 2,))],
        compiler_params=pltpu.CompilerParams(vmem_limit_bytes=16 * 1024 * 1024),
    )(rows, hi, lo, place, ids, offsets)


LEVELS = 4
POOL = 46


def local(embeddings, lists, row_ids, centroids, rotation):
    row_count, width = embeddings.shape
    owned = centroids.shape[0]
    n = lax.axis_size("dev")
    cap = 2 * row_count
    real = cap // n
    near = LANES // n
    direct = (7 * real + 8) // 16
    late, extra = direct - near, real - direct
    members = n // LEVELS
    pool = POOL
    block = -(-(pool + 1) // 16) * 16
    tall = width // LANES
    by_lane = (row_count // LANES, LANES)
    vmem = pl.BlockSpec(memory_space=pltpu.VMEM)
    hbm = pl.BlockSpec(memory_space=pltpu.HBM)

    def rows_of(*lead):
        return pltpu.VMEM((*lead, tall, LANES), F32)

    packed, hi, lo, place, ids, offsets, most = pl.pallas_call(
        functools.partial(relayed_kernel, n, real, near, direct, pool),
        out_shape=(
            jax.ShapeDtypeStruct((cap, width), F32),
            jax.ShapeDtypeStruct((near * n, width), BF16),
            jax.ShapeDtypeStruct((near * n, width), BF16),
            jax.ShapeDtypeStruct((cap, near * n), BF16),
            jax.ShapeDtypeStruct((cap // LANES, LANES), jnp.int32),
            jax.ShapeDtypeStruct((owned // LANES, LANES), jnp.int32),
            jax.ShapeDtypeStruct((1, LANES), jnp.int32),
        ),
        in_specs=[hbm] * 5,
        out_specs=(vmem,) * 7,
        scratch_shapes=[
            pltpu.VMEM((row_count, width), F32),
            pltpu.VMEM(by_lane, jnp.int32),
            pltpu.VMEM(by_lane, jnp.int32),
            pltpu.VMEM((row_count, width), BF16),
            pltpu.VMEM((row_count, width), BF16),
            rows_of(late, n), rows_of(near, n), rows_of(extra, members), rows_of(block), rows_of(block), rows_of(block),
            pltpu.VMEM((n, 1, LANES), jnp.int32),
            rows_of(real, n), rows_of(block), rows_of(block), rows_of(block),
            pltpu.VMEM((n, 1, LANES), jnp.int32),
            rows_of(extra, members), rows_of(extra, members), rows_of(extra, members),
            pltpu.VMEM((owned, width), F32),
            pltpu.VMEM((width, width), F32),
            pltpu.VMEM((width, width), BF16),
            pltpu.VMEM((width, width), BF16),
            pltpu.VMEM((cap, width), F32),
            pltpu.VMEM((cap, width), BF16),
            pltpu.VMEM((cap, width), BF16),
            pltpu.VMEM((cap, n * real), BF16),
            pltpu.SemaphoreType.DMA((7,)),
            pltpu.SemaphoreType.DMA((7,)),
            pltpu.SemaphoreType.DMA((5,)),
        ],
        compiler_params=pltpu.CompilerParams(
            collective_id=0, has_side_effects=True, vmem_limit_bytes=48 * 1024 * 1024
        ),
    )(embeddings, lists.reshape(by_lane), row_ids.reshape(by_lane), centroids, rotation)
    packed, hi, lo = lax.cond(
        most[0, 0] > pool,
        lambda: (full(embeddings, lists, row_ids, centroids, rotation), jnp.zeros_like(hi), jnp.zeros_like(lo)),
        lambda: (packed, hi, lo),
    )
    packed, ids, offsets = finish(packed, hi, lo, place, ids, offsets)
    return packed, ids.reshape(-1), offsets.reshape(-1)


def solution(mesh):
    in_specs = (P("dev", None), P("dev"), P("dev"), P("dev", None), P())
    out_specs = (P("dev", None), P("dev"), P("dev"))
    return jax.shard_map(local, mesh=mesh, in_specs=in_specs, out_specs=out_specs, check_vma=False)
```

```python
import functools

import jax
import jax.numpy as jnp
from jax import lax
from jax.experimental import pallas as pl
from jax.experimental.pallas import tpu as pltpu
from jax.sharding import PartitionSpec as P

MESH = pl.DeviceIdType.MESH
F32 = jnp.float32
BF16 = jnp.bfloat16
LANES = 128


def split(x):
    hi = x.astype(BF16)
    lo = (x - hi.astype(F32)).astype(BF16)
    return hi, lo


def dot(a, b):
    return jnp.dot(a, b, preferred_element_type=F32)


def kernel(
    n, slots, chunks,
    send, meta, cent, rot,
    out, ids_out, off_out,
    recv, meta_in, cent_buf, rot_buf, rot_hi, rot_lo, res, place,
    send_sem, recv_sem, meta_send_sem, meta_recv_sem, own_sem, load_sem,
):
    me = lax.axis_index("dev")
    cap, width = out.shape
    owned = cent.shape[0]
    entries = n * slots
    groups = entries // LANES
    per = LANES // slots
    wide = width // chunks

    load_cent = pltpu.make_async_copy(cent, cent_buf, load_sem.at[0])
    load_rot = pltpu.make_async_copy(rot, rot_buf, load_sem.at[1])
    own_meta = pltpu.make_async_copy(meta.at[me], meta_in.at[me], own_sem.at[chunks])

    def own_rows(c):
        cols = pl.ds(pl.multiple_of(c * wide, wide), wide)
        return pltpu.make_async_copy(send.at[me, :, cols], recv.at[c, me], own_sem.at[c])

    barrier = pltpu.get_barrier_semaphore()

    def greet(k, carry):
        peer = lax.rem(me + k, n)
        pl.semaphore_signal(barrier, inc=1, device_id=(peer,), device_id_type=MESH)
        return carry

    lax.fori_loop(1, n, greet, 0)
    own_meta.start()
    pl.semaphore_wait(barrier, n - 1)

    def peer_of(j):
        k = n // 2 + (2 * lax.rem(j, 2) - 1) * lax.div(j + 1, 2)
        return lax.rem(me + k, n)

    def send_meta(j, carry):
        peer = peer_of(j)
        pltpu.make_async_remote_copy(
            src_ref=meta.at[peer], dst_ref=meta_in.at[me],
            send_sem=meta_send_sem, recv_sem=meta_recv_sem,
            device_id=(peer,), device_id_type=MESH,
        ).start()
        return carry

    lax.fori_loop(0, n - 1, send_meta, 0)

    for c in range(chunks):
        def send_rows(j, carry):
            peer = peer_of(j)
            pltpu.make_async_remote_copy(
                src_ref=send.at[peer, :, pl.ds(c * wide, wide)], dst_ref=recv.at[c, me],
                send_sem=send_sem.at[c], recv_sem=recv_sem.at[c],
                device_id=(peer,), device_id_type=MESH,
            ).start()
            return carry

        lax.fori_loop(0, n - 1, send_rows, 0)

    load_cent.start()
    load_rot.start()
    for c in range(chunks):
        own_rows(c).start()

    most = pl.ds(0, n - 1)
    pltpu.make_async_copy(meta_in.at[most], meta_in.at[most], meta_recv_sem).wait()
    own_meta.wait()

    list_row, id_row, key_row, key_col, list_col, id_col = [], [], [], [], [], []
    lane = lax.broadcasted_iota(jnp.int32, (1, LANES), 1)
    for g in range(groups):
        got = jnp.sum(meta_in[pl.ds(g * per, per)], axis=0)
        found = got[0:1] - 1
        safe = jnp.where(found >= 0, found, owned)
        key = safe * entries + (g * LANES) + lane
        list_row.append(safe)
        id_row.append(got[1:2])
        key_row.append(key)
        key_col.append(jnp.transpose(jnp.broadcast_to(key, (LANES, LANES))))
        list_col.append(jnp.transpose(jnp.broadcast_to(safe, (LANES, LANES))))
        id_col.append(jnp.transpose(jnp.broadcast_to(got[1:2], (LANES, LANES))))

    slot_at = lax.broadcasted_iota(jnp.int32, (cap, LANES), 0)
    slot_list = jnp.zeros((cap, LANES), jnp.int32)
    pos_col = []
    for g in range(groups):
        rank = jnp.zeros((1, LANES), jnp.int32)
        for h in range(groups):
            less = (key_col[h] < key_row[g]).astype(jnp.int32)
            rank = rank + jnp.sum(less, axis=0, keepdims=True)
        rank = jnp.where(list_row[g] < owned, rank, cap + entries)
        hit = slot_at == rank
        place[:, pl.ds(g * LANES, LANES)] = hit.astype(F32).astype(BF16)
        slot_list = slot_list + jnp.where(hit, list_row[g] + 1, 0)
        pos_col.append(jnp.transpose(jnp.broadcast_to(rank, (LANES, LANES))))
    at_list = jnp.sum(slot_list, axis=1, keepdims=True) - 1

    for q in range(cap // LANES):
        total = jnp.zeros((1, LANES), jnp.int32)
        for g in range(groups):
            hit = pos_col[g] == lane + q * LANES
            total = total + jnp.sum(jnp.where(hit, id_col[g] + 1, 0), axis=0, keepdims=True)
        ids_out[pl.ds(q, 1), :] = total - 1
    for q in range(owned // LANES):
        total = jnp.zeros((1, LANES), jnp.int32)
        for g in range(groups):
            less = (list_col[g] < lane + q * LANES).astype(jnp.int32)
            total = total + jnp.sum(less, axis=0, keepdims=True)
        off_out[pl.ds(q, 1), :] = total

    res[...] = jnp.zeros_like(res)
    load_cent.wait()
    step = 256

    def centre(t, carry):
        base = pl.multiple_of(t * step, step)
        table = lax.broadcasted_iota(jnp.int32, (cap, step), 1) + base
        pick = (table == at_list).astype(F32).astype(BF16)
        for c in range(chunks):
            cols = pl.ds(c * wide, wide)
            hi, lo = split(cent_buf[pl.ds(base, step), cols])
            res[:, cols] -= dot(pick, hi) + dot(pick, lo)
        return carry

    lax.fori_loop(0, owned // step, centre, 0)

    load_rot.wait()

    def halve(t, carry):
        rows = pl.ds(pl.multiple_of(t * LANES, LANES), LANES)
        hi, lo = split(rot_buf[rows, :])
        rot_hi[rows, :] = hi
        rot_lo[rows, :] = lo
        return carry

    lax.fori_loop(0, width // LANES, halve, 0)
    out[...] = jnp.zeros_like(out)

    def turn(c, carry):
        pltpu.make_async_copy(recv.at[c, most], recv.at[c, most], recv_sem.at[c]).wait()
        own_rows(c).wait()
        cols = pl.ds(pl.multiple_of(c * wide, wide), wide)
        hi, lo = split(recv[c].reshape(entries, wide))
        spots = place[...]
        left = res[:, cols] + (dot(spots, hi) + dot(spots, lo))
        left_hi, left_lo = split(left)

        def tile(t, inner):
            at = pl.ds(pl.multiple_of(t * 256, 256), 256)
            r_hi = rot_hi[cols, at]
            r_lo = rot_lo[cols, at]
            out[:, at] += dot(left_hi, r_hi) + dot(left_lo, r_hi) + dot(left_hi, r_lo)
            return inner

        lax.fori_loop(0, width // 256, tile, 0)
        return carry

    lax.fori_loop(0, chunks, turn, 0)

    pltpu.make_async_copy(meta_in.at[most], meta_in.at[most], meta_send_sem).wait()
    for c in range(chunks):
        pltpu.make_async_copy(recv.at[c, most], recv.at[c, most], send_sem.at[c]).wait()


def full(embeddings, lists, row_ids, centroids, rotation):
    rows, width = embeddings.shape
    owned = centroids.shape[0]
    n = lax.axis_size("dev")
    cap = 2 * rows
    slots = max(8, cap // n)
    chunks = 4
    entries = n * slots
    me = lax.axis_index("dev")
    owner = lists // owned
    index = jnp.arange(rows, dtype=jnp.int32)
    earlier = index[None, :] < index[:, None]
    slot = jnp.sum((owner[None, :] == owner[:, None]) & earlier, axis=1).astype(jnp.int32)
    target = owner * slots + slot
    table = jnp.arange(entries, dtype=jnp.int32)
    match = target[None, :] == table[:, None]
    send = jnp.dot(match.astype(F32), embeddings, precision=lax.Precision.HIGH, preferred_element_type=F32)
    send = send.reshape(n, slots, width)
    per = LANES // slots
    own_lanes = (jnp.arange(LANES, dtype=jnp.int32) // slots) == lax.rem(me, per)

    def spread(values):
        picked = jnp.sum(jnp.where(match, values[None, :], 0), axis=1).astype(jnp.int32)
        return jnp.where(own_lanes[None, :], jnp.tile(picked.reshape(n, slots), (1, per)), 0)

    meta = jnp.zeros((n, 8, LANES), jnp.int32)
    meta = jnp.stack([spread(lists - owner * owned + 1), spread(row_ids)] + [jnp.zeros((n, LANES), jnp.int32)] * 6, axis=1)
    wide = width // chunks
    vmem = pl.BlockSpec(memory_space=pltpu.VMEM)
    hbm = pl.BlockSpec(memory_space=pltpu.HBM)
    packed, ids, offsets = pl.pallas_call(
        functools.partial(kernel, n, slots, chunks),
        out_shape=(
            jax.ShapeDtypeStruct((cap, width), F32),
            jax.ShapeDtypeStruct((cap // LANES, LANES), jnp.int32),
            jax.ShapeDtypeStruct((owned // LANES, LANES), jnp.int32),
        ),
        in_specs=[hbm, hbm, hbm, hbm],
        out_specs=(vmem, vmem, vmem),
        scratch_shapes=[
            pltpu.VMEM((chunks, n, slots, wide), F32),
            pltpu.VMEM((n, 8, LANES), jnp.int32),
            pltpu.VMEM((owned, width), F32),
            pltpu.VMEM((width, width), F32),
            pltpu.VMEM((width, width), BF16),
            pltpu.VMEM((width, width), BF16),
            pltpu.VMEM((cap, width), F32),
            pltpu.VMEM((cap, entries), BF16),
            pltpu.SemaphoreType.DMA((chunks,)),
            pltpu.SemaphoreType.DMA((chunks,)),
            pltpu.SemaphoreType.DMA,
            pltpu.SemaphoreType.DMA,
            pltpu.SemaphoreType.DMA((chunks + 1,)),
            pltpu.SemaphoreType.DMA((2,)),
        ],
        compiler_params=pltpu.CompilerParams(
            collective_id=1, has_side_effects=True, vmem_limit_bytes=36 * 1024 * 1024
        ),
    )(send, meta, centroids, rotation)
    return packed


def dot_t(a, b):
    return lax.dot_general(a, b, (((1,), (1,)), ((), ())), preferred_element_type=F32)


def hot(mask):
    return mask.astype(F32).astype(BF16)


def column_of(row):
    return jnp.transpose(jnp.broadcast_to(row, (LANES, LANES)))


def relayed_kernel(
    n, real, near, direct, pool, small,
    emb_hbm, lists_hbm, ids_hbm, cent, rot,
    out, last, last_place, ids_out, off_out, most_out, emb_out,
    emb, lists, ids, turned_hi, turned_lo, send_a, send_b, send_x, far_out, near_out, meta, recv, far_in, near_in, meta_in,
    part_1, part_2, part_3, cent_buf, rot_buf, rot_hi, rot_lo, res, left, place,
    send_sem, recv_sem, load_sem,
):
    me = lax.axis_index("dev")
    count, width = emb.shape
    cap = out.shape[0]
    owned = cent.shape[0]
    tall = width // LANES
    parts = count // LANES
    entries = n * real
    groups = entries // LANES
    members = n // LEVELS
    late = direct - near
    extra = real - direct
    soon = (near + 1) // 2
    block, block_near = far_in.shape[0], near_in.shape[0]
    level = lax.div(me, members)
    inside = lax.rem(me, members)
    beside = level + 1 - 2 * lax.rem(level, 2)
    across = lax.rem(level + 2, LEVELS)
    corner = lax.rem(beside + 2, LEVELS)
    META, A, B, X, FAR, NEAR = range(6)

    def flat(ref):
        return ref.reshape(ref.shape[0] * ref.shape[1] * tall, LANES) if len(ref.shape) == 4 else ref.reshape(ref.shape[0] * tall, LANES)

    recv_f, send_a_f, send_b_f, send_x_f = flat(recv), flat(send_a), flat(send_b), flat(send_x)
    far_out_f, near_out_f, far_in_f, near_in_f = flat(far_out), flat(near_out), flat(far_in), flat(near_in)
    part_1_f, part_2_f, part_3_f = flat(part_1), flat(part_2), flat(part_3)

    def tile_of(index):
        return pl.ds(pl.multiple_of(index * tall, 8), tall)

    load_cent = pltpu.make_async_copy(cent, cent_buf, load_sem.at[0])
    load_rot = pltpu.make_async_copy(rot, rot_buf, load_sem.at[1])
    barrier = pltpu.get_barrier_semaphore()

    def greet(k, carry):
        peer = lax.rem(me + k, n)
        pl.semaphore_signal(barrier, inc=1, device_id=(peer,), device_id_type=MESH)
        return carry

    lax.fori_loop(1, n, greet, 0)
    loads = [
        pltpu.make_async_copy(src, dst, load_sem.at[2 + k])
        for k, (src, dst) in enumerate(((lists_hbm, lists), (ids_hbm, ids), (emb_hbm, emb)))
    ]
    for load in loads:
        load.start()
    load_rot.start()
    for load in loads:
        load.wait()

    lane = lax.broadcasted_iota(jnp.int32, (1, LANES), 1)
    lanes = lax.broadcasted_iota(jnp.int32, (LANES, LANES), 1)
    subs = lax.broadcasted_iota(jnp.int32, (LANES, LANES), 0)
    ahead = subs < lanes

    list_of = [lists[r:r + 1, :] for r in range(parts)]
    id_of = [ids[r:r + 1, :] for r in range(parts)]
    owner_of = [lax.div(x, owned) for x in list_of]
    owner_col = [column_of(x) for x in owner_of]
    slot_of = []
    for r in range(parts):
        slot = jnp.zeros((1, LANES), jnp.int32)
        for q in range(r + 1):
            same = owner_col[q] == owner_of[r]
            if q == r:
                same = same & ahead
            slot = slot + jnp.sum(same.astype(jnp.int32), axis=0, keepdims=True)
        slot_of.append(slot)
    level_of = [lax.div(x, members) for x in owner_of]
    late_of = [slot_of[r] >= direct for r in range(parts)]
    home = [late_of[r] & (level_of[r] == level) for r in range(parts)]
    side = [late_of[r] & (level_of[r] == beside) for r in range(parts)]
    turn = [late_of[r] & (level_of[r] == corner) for r in range(parts)]
    gone = [late_of[r] & ((level_of[r] == across) | (level_of[r] == corner)) for r in range(parts)]
    seat = lax.broadcasted_iota(jnp.int32, (8, LANES), 0)
    triangle = hot(ahead)
    done = jnp.zeros((8, 1), F32)
    side_at, gone_at = [], []
    for r in range(parts):
        mask = ((seat == 0) & side[r]) | ((seat == 1) & gone[r])
        flags = mask.astype(F32)
        index = (dot(flags.astype(BF16), triangle) + done).astype(jnp.int32)
        done = done + jnp.sum(flags, axis=1, keepdims=True)
        side_at.append(jnp.where(side[r], index[0:1], -1))
        gone_at.append(jnp.where(gone[r], index[1:2], -1))
    worst = jnp.maximum(done[0:1] + (pool - small), done[1:2]).astype(jnp.int32)

    table = lax.broadcasted_iota(jnp.int32, (block + block_near, LANES), 0)
    picks = []
    for r in range(parts):
        target = jnp.where((gone_at[r] >= 0) & (gone_at[r] < pool), gone_at[r], -1)
        target = jnp.where((side_at[r] >= 0) & (side_at[r] < small), block + side_at[r], target)
        picks.append(hot(table == target))
    pick = jnp.concatenate(picks, axis=1)
    for b in range(0, tall, 2):
        hi, lo = split(emb[:, b * LANES:(b + 2) * LANES])
        left[pl.ds(0, count), pl.ds(b * LANES, 2 * LANES)] = hi
        left[pl.ds(count, count), pl.ds(b * LANES, 2 * LANES)] = lo
        value = dot(pick, hi) + dot(pick, lo)
        for h in range(2):
            got = value[:, h * LANES:(h + 1) * LANES]
            far_out_f[pl.ds(b + h, block, stride=tall), :] = got[:block]
            near_out_f[pl.ds(b + h, block_near, stride=tall), :] = got[block:]

    far_codes = jnp.zeros((8, LANES), F32)
    near_codes = jnp.zeros((8, LANES), F32)
    for r in range(parts):
        spot = (slot_of[r] - direct) * members + lax.rem(owner_of[r], members) + 1
        beyond = spot + jnp.where(turn[r], extra * members, 0)
        far_row = jnp.broadcast_to(beyond, (8, LANES)).astype(F32).astype(BF16)
        near_row = jnp.broadcast_to(spot, (8, LANES)).astype(F32).astype(BF16)
        far_codes = far_codes + dot_t(far_row, hot(subs == gone_at[r]))
        near_codes = near_codes + dot_t(near_row, hot(subs == side_at[r]))
    far_out[pool] = far_codes - 1.0
    near_out[small] = near_codes - 1.0
    blank = jnp.zeros((8, LANES), F32)
    for ref, used in ((far_in, pool + 1), (near_in, small + 1)):
        for k in range(used, ref.shape[0]):
            ref[k] = blank

    owners = lax.broadcasted_iota(jnp.int32, (n, LANES), 0)
    high = jnp.zeros((n, LANES), F32)
    low = jnp.zeros((n, LANES), F32)
    for r in range(parts):
        mine = owners == owner_of[r]
        local = list_of[r] - owner_of[r] * owned + 1
        for values, shift in ((local, 0), (id_of[r], real)):
            spots = hot(subs == slot_of[r] + shift)
            upper = lax.div(values, 256)
            lower = values - upper * 256
            high = high + dot_t(jnp.where(mine, upper, 0).astype(F32).astype(BF16), spots)
            low = low + dot_t(jnp.where(mine, lower, 0).astype(F32).astype(BF16), spots)
    note = high.astype(jnp.int32) * 256 + low.astype(jnp.int32)
    meta[:, 0, :] = jnp.where(lane == 2 * real, worst, note)

    meta_in[pl.ds(me, 1)] = meta[pl.ds(me, 1)]
    pl.semaphore_wait(barrier, n - 1)

    def post(src, dst, peer, at):
        pltpu.make_async_remote_copy(
            src_ref=src, dst_ref=dst, send_sem=send_sem.at[at], recv_sem=recv_sem.at[at],
            device_id=(peer,), device_id_type=MESH,
        ).start()

    def settle(ref, sem):
        pltpu.make_async_copy(ref, ref, sem).wait()

    def flips(bits):
        steps = []
        for bit in bits:
            steps.append(bit - 2 * bit * lax.rem(lax.div(me, bit), 2))
        return steps

    low_bits = [1, 2, 4]
    high_bits = [8 << k for k in range((n // 8).bit_length() - 1)]
    low_steps, high_steps = flips(low_bits), flips(high_bits)

    def to_peers(send):
        def eight(base, first):
            for k in range(first, 8):
                peer = base
                for bit, step in zip(low_bits, low_steps):
                    if k & bit:
                        peer = peer + step
                send(peer)

        def block_of(c, carry):
            base = me
            for k, step in enumerate(high_steps):
                base = base + step * lax.rem(lax.div(c, 1 << k), 2)
            eight(base, 0)
            return carry

        eight(me, 1)
        lax.fori_loop(1, n // 8, block_of, 0)

    def send_meta(peer):
        post(meta.at[peer], meta_in.at[me], peer, META)

    def send_first(peer):
        post(send_a.at[:, peer], recv.at[pl.ds(near, late), me], peer, A)

    def send_second(first, size):
        lines = pl.ds(first, size)

        def send(peer):
            post(send_b.at[lines, peer], recv.at[lines, me], peer, B)

        return send

    def spread(ref, source):
        def one(k, carry):
            other = lax.rem(inside + k, members)
            post(ref.at[:, other], recv.at[pl.ds(direct, extra), source], level * members + other, X)
            return carry
        lax.fori_loop(1, members, one, 0)

    far_message, near_message = pl.ds(0, pool + 1), pl.ds(0, small + 1)
    beside_dev = beside * members + inside
    across_dev = across * members + inside
    corner_dev = corner * members + inside

    post(far_out.at[far_message], far_in.at[far_message], across_dev, FAR)
    post(near_out.at[near_message], near_in.at[near_message], beside_dev, NEAR)
    to_peers(send_meta)
    load_rot.wait()
    load_cent.start()

    def halve(t, carry):
        at = pl.ds(pl.multiple_of(t * LANES, LANES), LANES)
        hi, lo = split(rot_buf[at, :])
        rot_hi[at, :] = hi
        rot_lo[at, :] = lo
        return carry

    lax.fori_loop(0, width // LANES, halve, 0)

    def turn_rows(rows):
        both, top = pl.ds(0, 2 * rows), pl.ds(0, rows)

        def turned(t, carry):
            at = pl.ds(pl.multiple_of(t * 256, 256), 256)
            value = dot(left[both, :], rot_hi[:, at])
            hi, lo = split(value[:rows] + value[rows:] + dot(left[top, :], rot_lo[:, at]))
            turned_hi[top, at] = hi
            turned_lo[top, at] = lo
            return carry

        lax.fori_loop(0, width // 256, turned, 0)

    turn_rows(count)
    base_x = late * n
    base_b = base_x + extra * members
    wanted = base_b + near * n
    table = lax.broadcasted_iota(jnp.int32, (wanted, LANES), 0)
    picks = []
    for r in range(parts):
        owner, slot = owner_of[r], slot_of[r]
        spot = (slot - direct) * members + lax.rem(owner, members)
        target = jnp.where(slot < direct, (slot - near) * n + owner, -1)
        target = jnp.where(slot < near, base_b + slot * n + owner, target)
        target = jnp.where(home[r], base_x + spot, target)
        picks.append(hot(table == target))
    pick = jnp.concatenate(picks, axis=1)
    for b in range(0, tall, 2):
        cols = pl.ds(b * LANES, 2 * LANES)
        value = dot(pick, turned_hi[:, cols]) + dot(pick, turned_lo[:, cols])
        for h in range(2):
            got = value[:, h * LANES:(h + 1) * LANES]
            send_a_f[pl.ds(b + h, late * n, stride=tall), :] = got[:base_x]
            send_x_f[pl.ds(b + h, extra * members, stride=tall), :] = got[base_x:base_b]
            send_b_f[pl.ds(b + h, near * n, stride=tall), :] = got[base_b:]
    to_peers(send_first)
    spread(send_x, me)
    to_peers(send_second(0, soon))
    for s in range(late):
        recv_f[tile_of((near + s) * n + me), :] = send_a_f[tile_of(s * n + me), :]
    for s in range(near):
        recv_f[tile_of(s * n + me), :] = send_b_f[tile_of(s * n + me), :]
    for s in range(extra):
        recv_f[tile_of((direct + s) * n + me), :] = send_x_f[tile_of(s * members + inside), :]

    keep_emb = pltpu.make_async_copy(emb, emb_out, load_sem.at[5])
    keep_emb.start()
    span_meta = meta_in.at[pl.ds(0, n - 1)]
    settle(span_meta, recv_sem.at[META])

    got = meta_in[:, 0, :]
    if n < LANES:
        got = jnp.concatenate([got, jnp.zeros((LANES - n, LANES), jnp.int32)], axis=0)
    fields = jnp.transpose(got)
    most_out[...] = jnp.broadcast_to(jnp.max(fields[2 * real:2 * real + 1, :], axis=1, keepdims=True), (1, LANES))
    per = LANES // n
    rolled = [fields if k == 0 else pltpu.roll(fields, n * k, 1) for k in range(per)]

    def row_of(g, first):
        total = jnp.zeros((1, LANES), jnp.int32)
        for k in range(per):
            at = first + g * per + k
            total = total + rolled[k][at:at + 1, :]
        return total

    list_row, key_row, key_col, list_col, id_col = [], [], [], [], []
    for g in range(groups):
        found = row_of(g, 0) - 1
        safe = jnp.where(found >= 0, found, owned)
        entry = g * LANES + lane
        key = safe * entries + lax.rem(entry, n) * real + lax.div(entry, n)
        list_row.append(safe)
        key_row.append(key)
        key_col.append(column_of(key))
        list_col.append(column_of(safe))
        id_col.append(column_of(row_of(g, real)))

    slot_at = lax.broadcasted_iota(jnp.int32, (cap, LANES), 0)
    slot_list = jnp.zeros((cap, LANES), jnp.int32)
    pos_col = []
    for g in range(groups):
        rank = jnp.zeros((1, LANES), jnp.int32)
        for h in range(groups):
            less = (key_col[h] < key_row[g]).astype(jnp.int32)
            rank = rank + jnp.sum(less, axis=0, keepdims=True)
        rank = jnp.where(list_row[g] < owned, rank, cap + entries)
        hit = slot_at == rank
        place[:, pl.ds(g * LANES, LANES)] = hot(hit)
        slot_list = slot_list + jnp.where(hit, list_row[g] + 1, 0)
        pos_col.append(column_of(rank))
    at_list = jnp.sum(slot_list, axis=1, keepdims=True) - 1

    def piece(ref, first, rows, b):
        return ref[pl.ds(first * tall + b, rows, stride=tall), :]

    def pair(ref, first, rows, b):
        return split(jnp.concatenate([piece(ref, first, rows, b), piece(ref, first, rows, b + 1)], axis=1))

    def expand(source, rows, used, targets):
        high = len(targets) * extra * members
        code = source[pl.ds(used * tall, 1), :][:, :rows].astype(jnp.int32)
        choose = hot(lax.broadcasted_iota(jnp.int32, (high, rows), 0) == code)
        for b in range(0, tall, 2):
            cols = pl.ds(b * LANES, 2 * LANES)
            hi, lo = pair(source, 0, rows, b)
            left[pl.ds(0, rows), cols] = hi
            left[pl.ds(rows, rows), cols] = lo
        turn_rows(rows)
        for b in range(0, tall, 2):
            cols = pl.ds(b * LANES, 2 * LANES)
            value = dot(choose, turned_hi[pl.ds(0, rows), cols]) + dot(choose, turned_lo[pl.ds(0, rows), cols])
            for k, target in enumerate(targets):
                for h in range(2):
                    part = value[k * extra * members:(k + 1) * extra * members, h * LANES:(h + 1) * LANES]
                    target[pl.ds(b + h, extra * members, stride=tall), :] = part

    def keep(ref, source):
        for s in range(extra):
            recv_f[tile_of((direct + s) * n + source), :] = ref[tile_of(s * members + inside), :]

    settle(near_in.at[near_message], recv_sem.at[NEAR])
    expand(near_in_f, block_near, small, [part_1_f])
    spread(part_1, beside_dev)
    keep(part_1_f, beside_dev)

    settle(far_in.at[far_message], recv_sem.at[FAR])
    expand(far_in_f, block, pool, [part_2_f, part_3_f])

    def send_over(k, carry):
        other = lax.rem(inside + k, members)
        post(part_3.at[:, other], recv.at[pl.ds(direct, extra), across_dev], beside * members + other, X)
        return carry

    lax.fori_loop(0, members, send_over, 0)
    spread(part_2, across_dev)
    keep(part_2_f, across_dev)
    if near > soon:
        to_peers(send_second(soon, near - soon))

    for q in range(cap // LANES):
        total = jnp.zeros((1, LANES), jnp.int32)
        for g in range(groups):
            hit = pos_col[g] == lane + q * LANES
            total = total + jnp.sum(jnp.where(hit, id_col[g] + 1, 0), axis=0, keepdims=True)
        ids_out[pl.ds(q, 1), :] = total - 1
    for q in range(owned // LANES):
        total = jnp.zeros((1, LANES), jnp.int32)
        for g in range(groups):
            less = (list_col[g] < lane + q * LANES).astype(jnp.int32)
            total = total + jnp.sum(less, axis=0, keepdims=True)
        off_out[pl.ds(q, 1), :] = total

    res[...] = jnp.zeros_like(res)
    load_cent.wait()
    step = 256

    def centre(t, carry):
        base = pl.multiple_of(t * step, step)
        table = lax.broadcasted_iota(jnp.int32, (cap, step), 1) + base
        pick = hot(table == at_list)
        for c in range(width // step):
            cols = pl.ds(c * step, step)
            hi, lo = split(cent_buf[pl.ds(base, step), cols])
            res[:, cols] -= dot(pick, hi) + dot(pick, lo)
        return carry

    lax.fori_loop(0, owned // step, centre, 0)

    for b in range(0, tall, 2):
        cols = pl.ds(b * LANES, 2 * LANES)
        hi, lo = split(res[:, cols])
        left[pl.ds(0, cap), cols] = hi
        left[pl.ds(cap, cap), cols] = lo

    def tile(t, carry):
        at = pl.ds(pl.multiple_of(t * 256, 256), 256)
        r_hi = rot_hi[:, at]
        top, low = left[pl.ds(0, cap), :], left[pl.ds(cap, cap), :]
        out[:, at] = dot(top, r_hi) + dot(low, r_hi) + dot(top, rot_lo[:, at])
        return carry

    lax.fori_loop(0, width // 256, tile, 0)

    span_a = recv.at[pl.ds(near, late), pl.ds(0, n - 1)]
    settle(span_a, recv_sem.at[A])
    span_x = recv_f.at[pl.ds(0, extra * (LEVELS * members - LEVELS + 1) * tall)]
    settle(span_x, recv_sem.at[X])
    rest = entries - near * n
    for b in range(0, tall, 2):
        cols = pl.ds(b * LANES, 2 * LANES)
        hi, lo = pair(recv_f, near * n, rest, b)
        spots = place[:, near * n:]
        out[:, cols] += dot(spots, hi) + dot(spots, lo)

    span_b = recv.at[pl.ds(0, near), pl.ds(0, n - 1)]
    last_place[:, :near * n] = place[:, :near * n]
    last_place[:, near * n:] = place[:, :near * n]
    settle(span_b, recv_sem.at[B])
    for b in range(0, tall, 2):
        cols = pl.ds(b * LANES, 2 * LANES)
        hi, lo = pair(recv_f, 0, near * n, b)
        last[pl.ds(0, near * n), cols] = hi
        last[pl.ds(near * n, near * n), cols] = lo

    keep_emb.wait()
    settle(span_meta, send_sem.at[META])
    settle(span_a, send_sem.at[A])
    settle(span_b, send_sem.at[B])
    settle(span_x, send_sem.at[X])
    settle(far_in.at[far_message], send_sem.at[FAR])
    settle(near_in.at[near_message], send_sem.at[NEAR])


def finish_kernel(pool, most, rows, last, place, ids, offsets, rows_out, ids_out, off_out, buf, sem):
    wide = 256
    tiles = rows.shape[1] // wide
    moves = [
        pltpu.make_async_copy(ids, ids_out, sem.at[tiles]),
        pltpu.make_async_copy(offsets, off_out, sem.at[tiles + 1]),
    ]
    for move in moves:
        move.start()
    for t in range(tiles):
        cols = pl.ds(t * wide, wide)
        kept = rows[:, cols]
        buf[t] = jnp.where(most[0:1, 0:1] > pool, kept, kept + dot(place[...], last[:, cols]))
        move = pltpu.make_async_copy(buf.at[t], rows_out.at[:, cols], sem.at[t])
        move.start()
        moves.append(move)
    for move in moves:
        move.wait()


def finish(pool, most, rows, last, place, ids, offsets):
    vmem = pl.BlockSpec(memory_space=pltpu.VMEM)
    hbm = pl.BlockSpec(memory_space=pltpu.HBM)
    cap, width = rows.shape
    return pl.pallas_call(
        functools.partial(finish_kernel, pool),
        out_shape=tuple(jax.ShapeDtypeStruct(x.shape, x.dtype) for x in (rows, ids, offsets)),
        in_specs=[vmem] * 6,
        out_specs=(hbm,) * 3,
        scratch_shapes=[pltpu.VMEM((width // 256, cap, 256), F32), pltpu.SemaphoreType.DMA((width // 256 + 2,))],
        compiler_params=pltpu.CompilerParams(vmem_limit_bytes=8 * 1024 * 1024),
    )(most, rows, last, place, ids, offsets)


LEVELS = 4
POOL = 44
SMALL = 34


def local(embeddings, lists, row_ids, centroids, rotation):
    row_count, width = embeddings.shape
    owned = centroids.shape[0]
    n = lax.axis_size("dev")
    cap = 2 * row_count
    real = cap // n
    near = LANES // n
    direct = (7 * real + 8) // 16
    late, extra = direct - near, real - direct
    members = n // LEVELS
    pool, small = POOL, SMALL
    block, block_near = -(-(pool + 1) // 16) * 16, -(-(small + 1) // 16) * 16
    tall = width // LANES
    by_lane = (row_count // LANES, LANES)
    vmem = pl.BlockSpec(memory_space=pltpu.VMEM)
    hbm = pl.BlockSpec(memory_space=pltpu.HBM)

    def rows_of(*lead):
        return pltpu.VMEM((*lead, tall, LANES), F32)

    packed, last, place, ids, offsets, most, copied = pl.pallas_call(
        functools.partial(relayed_kernel, n, real, near, direct, pool, small),
        out_shape=(
            jax.ShapeDtypeStruct((cap, width), F32),
            jax.ShapeDtypeStruct((2 * near * n, width), BF16),
            jax.ShapeDtypeStruct((cap, 2 * near * n), BF16),
            jax.ShapeDtypeStruct((cap // LANES, LANES), jnp.int32),
            jax.ShapeDtypeStruct((owned // LANES, LANES), jnp.int32),
            jax.ShapeDtypeStruct((1, LANES), jnp.int32),
            jax.ShapeDtypeStruct((row_count, width), F32),
        ),
        in_specs=[hbm] * 5,
        out_specs=(vmem,) * 6 + (hbm,),
        scratch_shapes=[
            pltpu.VMEM((row_count, width), F32),
            pltpu.VMEM(by_lane, jnp.int32),
            pltpu.VMEM(by_lane, jnp.int32),
            pltpu.VMEM((row_count, width), BF16),
            pltpu.VMEM((row_count, width), BF16),
            rows_of(late, n), rows_of(near, n), rows_of(extra, members), rows_of(block), rows_of(block_near),
            pltpu.VMEM((n, 1, LANES), jnp.int32),
            rows_of(real, n), rows_of(block), rows_of(block_near),
            pltpu.VMEM((n, 1, LANES), jnp.int32),
            rows_of(extra, members), rows_of(extra, members), rows_of(extra, members),
            pltpu.VMEM((owned, width), F32),
            pltpu.VMEM((width, width), F32),
            pltpu.VMEM((width, width), BF16),
            pltpu.VMEM((width, width), BF16),
            pltpu.VMEM((cap, width), F32),
            pltpu.VMEM((2 * cap, width), BF16),
            pltpu.VMEM((cap, n * real), BF16),
            pltpu.SemaphoreType.DMA((6,)),
            pltpu.SemaphoreType.DMA((6,)),
            pltpu.SemaphoreType.DMA((6,)),
        ],
        compiler_params=pltpu.CompilerParams(
            collective_id=0, has_side_effects=True, vmem_limit_bytes=36 * 1024 * 1024
        ),
    )(embeddings, lists.reshape(by_lane), row_ids.reshape(by_lane), centroids, rotation)
    packed = lax.cond(
        most[0, 0] > pool,
        lambda: full(copied, lists, row_ids, centroids, rotation),
        lambda: packed,
    )
    packed, ids, offsets = finish(pool, most, packed, last, place, ids, offsets)
    return packed, ids.reshape(-1), offsets.reshape(-1)


def solution(mesh):
    in_specs = (P("dev", None), P("dev"), P("dev"), P("dev", None), P())
    out_specs = (P("dev", None), P("dev"), P("dev"))
    return jax.shard_map(local, mesh=mesh, in_specs=in_specs, out_specs=out_specs, check_vma=False)
```

```python
import functools

import jax
import jax.numpy as jnp
from jax import lax
from jax.experimental import pallas as pl
from jax.experimental.pallas import tpu as pltpu
from jax.sharding import PartitionSpec as P

MESH = pl.DeviceIdType.MESH
F32 = jnp.float32
BF16 = jnp.bfloat16
LANES = 128


def split(x):
    hi = x.astype(BF16)
    lo = (x - hi.astype(F32)).astype(BF16)
    return hi, lo


def dot(a, b):
    return jnp.dot(a, b, preferred_element_type=F32)


def kernel(
    n, slots, chunks,
    send, meta, cent, rot,
    out, ids_out, off_out,
    recv, meta_in, cent_buf, rot_buf, rot_hi, rot_lo, res, place,
    send_sem, recv_sem, meta_send_sem, meta_recv_sem, own_sem, load_sem,
):
    me = lax.axis_index("dev")
    cap, width = out.shape
    owned = cent.shape[0]
    entries = n * slots
    groups = entries // LANES
    per = LANES // slots
    wide = width // chunks

    load_cent = pltpu.make_async_copy(cent, cent_buf, load_sem.at[0])
    load_rot = pltpu.make_async_copy(rot, rot_buf, load_sem.at[1])
    own_meta = pltpu.make_async_copy(meta.at[me], meta_in.at[me], own_sem.at[chunks])

    def own_rows(c):
        cols = pl.ds(pl.multiple_of(c * wide, wide), wide)
        return pltpu.make_async_copy(send.at[me, :, cols], recv.at[c, me], own_sem.at[c])

    barrier = pltpu.get_barrier_semaphore()

    def greet(k, carry):
        peer = lax.rem(me + k, n)
        pl.semaphore_signal(barrier, inc=1, device_id=(peer,), device_id_type=MESH)
        return carry

    lax.fori_loop(1, n, greet, 0)
    own_meta.start()
    pl.semaphore_wait(barrier, n - 1)

    def peer_of(j):
        k = n // 2 + (2 * lax.rem(j, 2) - 1) * lax.div(j + 1, 2)
        return lax.rem(me + k, n)

    def send_meta(j, carry):
        peer = peer_of(j)
        pltpu.make_async_remote_copy(
            src_ref=meta.at[peer], dst_ref=meta_in.at[me],
            send_sem=meta_send_sem, recv_sem=meta_recv_sem,
            device_id=(peer,), device_id_type=MESH,
        ).start()
        return carry

    lax.fori_loop(0, n - 1, send_meta, 0)

    for c in range(chunks):
        def send_rows(j, carry):
            peer = peer_of(j)
            pltpu.make_async_remote_copy(
                src_ref=send.at[peer, :, pl.ds(c * wide, wide)], dst_ref=recv.at[c, me],
                send_sem=send_sem.at[c], recv_sem=recv_sem.at[c],
                device_id=(peer,), device_id_type=MESH,
            ).start()
            return carry

        lax.fori_loop(0, n - 1, send_rows, 0)

    load_cent.start()
    load_rot.start()
    for c in range(chunks):
        own_rows(c).start()

    most = pl.ds(0, n - 1)
    pltpu.make_async_copy(meta_in.at[most], meta_in.at[most], meta_recv_sem).wait()
    own_meta.wait()

    list_row, id_row, key_row, key_col, list_col, id_col = [], [], [], [], [], []
    lane = lax.broadcasted_iota(jnp.int32, (1, LANES), 1)
    for g in range(groups):
        got = jnp.sum(meta_in[pl.ds(g * per, per)], axis=0)
        found = got[0:1] - 1
        safe = jnp.where(found >= 0, found, owned)
        key = safe * entries + (g * LANES) + lane
        list_row.append(safe)
        id_row.append(got[1:2])
        key_row.append(key)
        key_col.append(jnp.transpose(jnp.broadcast_to(key, (LANES, LANES))))
        list_col.append(jnp.transpose(jnp.broadcast_to(safe, (LANES, LANES))))
        id_col.append(jnp.transpose(jnp.broadcast_to(got[1:2], (LANES, LANES))))

    slot_at = lax.broadcasted_iota(jnp.int32, (cap, LANES), 0)
    slot_list = jnp.zeros((cap, LANES), jnp.int32)
    pos_col = []
    for g in range(groups):
        rank = jnp.zeros((1, LANES), jnp.int32)
        for h in range(groups):
            less = (key_col[h] < key_row[g]).astype(jnp.int32)
            rank = rank + jnp.sum(less, axis=0, keepdims=True)
        rank = jnp.where(list_row[g] < owned, rank, cap + entries)
        hit = slot_at == rank
        place[:, pl.ds(g * LANES, LANES)] = hit.astype(F32).astype(BF16)
        slot_list = slot_list + jnp.where(hit, list_row[g] + 1, 0)
        pos_col.append(jnp.transpose(jnp.broadcast_to(rank, (LANES, LANES))))
    at_list = jnp.sum(slot_list, axis=1, keepdims=True) - 1

    for q in range(cap // LANES):
        total = jnp.zeros((1, LANES), jnp.int32)
        for g in range(groups):
            hit = pos_col[g] == lane + q * LANES
            total = total + jnp.sum(jnp.where(hit, id_col[g] + 1, 0), axis=0, keepdims=True)
        ids_out[pl.ds(q, 1), :] = total - 1
    for q in range(owned // LANES):
        total = jnp.zeros((1, LANES), jnp.int32)
        for g in range(groups):
            less = (list_col[g] < lane + q * LANES).astype(jnp.int32)
            total = total + jnp.sum(less, axis=0, keepdims=True)
        off_out[pl.ds(q, 1), :] = total

    res[...] = jnp.zeros_like(res)
    load_cent.wait()
    step = 256

    def centre(t, carry):
        base = pl.multiple_of(t * step, step)
        table = lax.broadcasted_iota(jnp.int32, (cap, step), 1) + base
        pick = (table == at_list).astype(F32).astype(BF16)
        for c in range(chunks):
            cols = pl.ds(c * wide, wide)
            hi, lo = split(cent_buf[pl.ds(base, step), cols])
            res[:, cols] -= dot(pick, hi) + dot(pick, lo)
        return carry

    lax.fori_loop(0, owned // step, centre, 0)

    load_rot.wait()

    def halve(t, carry):
        rows = pl.ds(pl.multiple_of(t * LANES, LANES), LANES)
        hi, lo = split(rot_buf[rows, :])
        rot_hi[rows, :] = hi
        rot_lo[rows, :] = lo
        return carry

    lax.fori_loop(0, width // LANES, halve, 0)
    out[...] = jnp.zeros_like(out)

    def turn(c, carry):
        pltpu.make_async_copy(recv.at[c, most], recv.at[c, most], recv_sem.at[c]).wait()
        own_rows(c).wait()
        cols = pl.ds(pl.multiple_of(c * wide, wide), wide)
        hi, lo = split(recv[c].reshape(entries, wide))
        spots = place[...]
        left = res[:, cols] + (dot(spots, hi) + dot(spots, lo))
        left_hi, left_lo = split(left)

        def tile(t, inner):
            at = pl.ds(pl.multiple_of(t * 256, 256), 256)
            r_hi = rot_hi[cols, at]
            r_lo = rot_lo[cols, at]
            out[:, at] += dot(left_hi, r_hi) + dot(left_lo, r_hi) + dot(left_hi, r_lo)
            return inner

        lax.fori_loop(0, width // 256, tile, 0)
        return carry

    lax.fori_loop(0, chunks, turn, 0)

    pltpu.make_async_copy(meta_in.at[most], meta_in.at[most], meta_send_sem).wait()
    for c in range(chunks):
        pltpu.make_async_copy(recv.at[c, most], recv.at[c, most], send_sem.at[c]).wait()


def full(embeddings, lists, row_ids, centroids, rotation):
    rows, width = embeddings.shape
    owned = centroids.shape[0]
    n = lax.axis_size("dev")
    cap = 2 * rows
    slots = max(8, cap // n)
    chunks = 4
    entries = n * slots
    me = lax.axis_index("dev")
    owner = lists // owned
    index = jnp.arange(rows, dtype=jnp.int32)
    earlier = index[None, :] < index[:, None]
    slot = jnp.sum((owner[None, :] == owner[:, None]) & earlier, axis=1).astype(jnp.int32)
    target = owner * slots + slot
    table = jnp.arange(entries, dtype=jnp.int32)
    match = target[None, :] == table[:, None]
    send = jnp.dot(match.astype(F32), embeddings, precision=lax.Precision.HIGH, preferred_element_type=F32)
    send = send.reshape(n, slots, width)
    per = LANES // slots
    own_lanes = (jnp.arange(LANES, dtype=jnp.int32) // slots) == lax.rem(me, per)

    def spread(values):
        picked = jnp.sum(jnp.where(match, values[None, :], 0), axis=1).astype(jnp.int32)
        return jnp.where(own_lanes[None, :], jnp.tile(picked.reshape(n, slots), (1, per)), 0)

    meta = jnp.zeros((n, 8, LANES), jnp.int32)
    meta = jnp.stack([spread(lists - owner * owned + 1), spread(row_ids)] + [jnp.zeros((n, LANES), jnp.int32)] * 6, axis=1)
    wide = width // chunks
    vmem = pl.BlockSpec(memory_space=pltpu.VMEM)
    hbm = pl.BlockSpec(memory_space=pltpu.HBM)
    packed, ids, offsets = pl.pallas_call(
        functools.partial(kernel, n, slots, chunks),
        out_shape=(
            jax.ShapeDtypeStruct((cap, width), F32),
            jax.ShapeDtypeStruct((cap // LANES, LANES), jnp.int32),
            jax.ShapeDtypeStruct((owned // LANES, LANES), jnp.int32),
        ),
        in_specs=[hbm, hbm, hbm, hbm],
        out_specs=(vmem, vmem, vmem),
        scratch_shapes=[
            pltpu.VMEM((chunks, n, slots, wide), F32),
            pltpu.VMEM((n, 8, LANES), jnp.int32),
            pltpu.VMEM((owned, width), F32),
            pltpu.VMEM((width, width), F32),
            pltpu.VMEM((width, width), BF16),
            pltpu.VMEM((width, width), BF16),
            pltpu.VMEM((cap, width), F32),
            pltpu.VMEM((cap, entries), BF16),
            pltpu.SemaphoreType.DMA((chunks,)),
            pltpu.SemaphoreType.DMA((chunks,)),
            pltpu.SemaphoreType.DMA,
            pltpu.SemaphoreType.DMA,
            pltpu.SemaphoreType.DMA((chunks + 1,)),
            pltpu.SemaphoreType.DMA((2,)),
        ],
        compiler_params=pltpu.CompilerParams(
            collective_id=1, has_side_effects=True, vmem_limit_bytes=36 * 1024 * 1024
        ),
    )(send, meta, centroids, rotation)
    return packed


def dot_t(a, b):
    return lax.dot_general(a, b, (((1,), (1,)), ((), ())), preferred_element_type=F32)


def hot(mask):
    return mask.astype(F32).astype(BF16)


def column_of(row):
    return jnp.transpose(jnp.broadcast_to(row, (LANES, LANES)))


def relayed_kernel(
    n, real, near, direct, pool, small,
    emb_hbm, lists_hbm, ids_hbm, cent, rot,
    out, last, last_place, ids_out, off_out, most_out, emb_out,
    emb, lists, ids, turned_hi, turned_lo, send_a, send_b, send_x, far_out, near_out, meta, recv, far_in, near_in, meta_in,
    part_1, part_2, part_3, cent_buf, rot_buf, rot_hi, rot_lo, res, left, place, place_twice,
    send_sem, recv_sem, load_sem,
):
    me = lax.axis_index("dev")
    count, width = emb.shape
    cap = out.shape[0]
    owned = cent.shape[0]
    tall = width // LANES
    parts = count // LANES
    entries = n * real
    groups = entries // LANES
    members = n // LEVELS
    late = direct - near
    extra = real - direct
    soon = (near + 1) // 2
    block, block_near = far_in.shape[0], near_in.shape[0]
    level = lax.div(me, members)
    inside = lax.rem(me, members)
    beside = level + 1 - 2 * lax.rem(level, 2)
    across = lax.rem(level + 2, LEVELS)
    corner = lax.rem(beside + 2, LEVELS)
    META, A, B, X, FAR, NEAR = range(6)

    def flat(ref):
        return ref.reshape(ref.shape[0] * ref.shape[1] * tall, LANES) if len(ref.shape) == 4 else ref.reshape(ref.shape[0] * tall, LANES)

    recv_f, send_a_f, send_b_f, send_x_f = flat(recv), flat(send_a), flat(send_b), flat(send_x)
    far_out_f, near_out_f, far_in_f, near_in_f = flat(far_out), flat(near_out), flat(far_in), flat(near_in)
    part_1_f, part_2_f, part_3_f = flat(part_1), flat(part_2), flat(part_3)

    def tile_of(index):
        return pl.ds(pl.multiple_of(index * tall, 8), tall)

    load_cent = pltpu.make_async_copy(cent, cent_buf, load_sem.at[0])
    load_rot = pltpu.make_async_copy(rot, rot_buf, load_sem.at[1])
    barrier = pltpu.get_barrier_semaphore()

    def greet(k, carry):
        peer = lax.rem(me + k, n)
        pl.semaphore_signal(barrier, inc=1, device_id=(peer,), device_id_type=MESH)
        return carry

    lax.fori_loop(1, n, greet, 0)
    loads = [
        pltpu.make_async_copy(src, dst, load_sem.at[2 + k])
        for k, (src, dst) in enumerate(((lists_hbm, lists), (ids_hbm, ids), (emb_hbm, emb)))
    ]
    for load in loads:
        load.start()
    load_rot.start()
    for load in loads:
        load.wait()

    lane = lax.broadcasted_iota(jnp.int32, (1, LANES), 1)
    lanes = lax.broadcasted_iota(jnp.int32, (LANES, LANES), 1)
    subs = lax.broadcasted_iota(jnp.int32, (LANES, LANES), 0)
    ahead = subs < lanes

    list_of = [lists[r:r + 1, :] for r in range(parts)]
    id_of = [ids[r:r + 1, :] for r in range(parts)]
    owner_of = [lax.div(x, owned) for x in list_of]
    owner_col = [column_of(x) for x in owner_of]
    slot_of = []
    for r in range(parts):
        slot = jnp.zeros((1, LANES), jnp.int32)
        for q in range(r + 1):
            same = owner_col[q] == owner_of[r]
            if q == r:
                same = same & ahead
            slot = slot + jnp.sum(same.astype(jnp.int32), axis=0, keepdims=True)
        slot_of.append(slot)
    level_of = [lax.div(x, members) for x in owner_of]
    late_of = [slot_of[r] >= direct for r in range(parts)]
    home = [late_of[r] & (level_of[r] == level) for r in range(parts)]
    side = [late_of[r] & (level_of[r] == beside) for r in range(parts)]
    turn = [late_of[r] & (level_of[r] == corner) for r in range(parts)]
    gone = [late_of[r] & ((level_of[r] == across) | (level_of[r] == corner)) for r in range(parts)]
    seat = lax.broadcasted_iota(jnp.int32, (8, LANES), 0)
    triangle = hot(ahead)
    done = jnp.zeros((8, 1), F32)
    side_at, gone_at = [], []
    for r in range(parts):
        mask = ((seat == 0) & side[r]) | ((seat == 1) & gone[r])
        flags = mask.astype(F32)
        index = (dot(flags.astype(BF16), triangle) + done).astype(jnp.int32)
        done = done + jnp.sum(flags, axis=1, keepdims=True)
        side_at.append(jnp.where(side[r], index[0:1], -1))
        gone_at.append(jnp.where(gone[r], index[1:2], -1))
    worst = jnp.maximum(done[0:1] + (pool - small), done[1:2]).astype(jnp.int32)

    table = lax.broadcasted_iota(jnp.int32, (block + block_near, LANES), 0)
    picks = []
    for r in range(parts):
        target = jnp.where((gone_at[r] >= 0) & (gone_at[r] < pool), gone_at[r], -1)
        target = jnp.where((side_at[r] >= 0) & (side_at[r] < small), block + side_at[r], target)
        picks.append(hot(table == target))
    pick = jnp.concatenate(picks, axis=1)
    for b in range(0, tall, 2):
        hi, lo = split(emb[:, b * LANES:(b + 2) * LANES])
        left[pl.ds(0, count), pl.ds(b * LANES, 2 * LANES)] = hi
        left[pl.ds(count, count), pl.ds(b * LANES, 2 * LANES)] = lo
        value = dot(pick, hi) + dot(pick, lo)
        for h in range(2):
            got = value[:, h * LANES:(h + 1) * LANES]
            far_out_f[pl.ds(b + h, block, stride=tall), :] = got[:block]
            near_out_f[pl.ds(b + h, block_near, stride=tall), :] = got[block:]

    far_codes = jnp.zeros((8, LANES), F32)
    near_codes = jnp.zeros((8, LANES), F32)
    for r in range(parts):
        spot = (slot_of[r] - direct) * members + lax.rem(owner_of[r], members) + 1
        beyond = spot + jnp.where(turn[r], extra * members, 0)
        far_row = jnp.broadcast_to(beyond, (8, LANES)).astype(F32).astype(BF16)
        near_row = jnp.broadcast_to(spot, (8, LANES)).astype(F32).astype(BF16)
        far_codes = far_codes + dot_t(far_row, hot(subs == gone_at[r]))
        near_codes = near_codes + dot_t(near_row, hot(subs == side_at[r]))
    far_out[pool] = far_codes - 1.0
    near_out[small] = near_codes - 1.0
    blank = jnp.zeros((8, LANES), F32)
    for ref, used in ((far_in, pool + 1), (near_in, small + 1)):
        for k in range(used, ref.shape[0]):
            ref[k] = blank

    owners = lax.broadcasted_iota(jnp.int32, (n, LANES), 0)
    high = jnp.zeros((n, LANES), F32)
    low = jnp.zeros((n, LANES), F32)
    for r in range(parts):
        mine = owners == owner_of[r]
        local = list_of[r] - owner_of[r] * owned + 1
        for values, shift in ((local, 0), (id_of[r], real)):
            spots = hot(subs == slot_of[r] + shift)
            upper = lax.div(values, 256)
            lower = values - upper * 256
            high = high + dot_t(jnp.where(mine, upper, 0).astype(F32).astype(BF16), spots)
            low = low + dot_t(jnp.where(mine, lower, 0).astype(F32).astype(BF16), spots)
    note = high.astype(jnp.int32) * 256 + low.astype(jnp.int32)
    meta[:, 0, :] = jnp.where(lane == 2 * real, worst, note)

    meta_in[pl.ds(me, 1)] = meta[pl.ds(me, 1)]
    pl.semaphore_wait(barrier, n - 1)

    def post(src, dst, peer, at):
        pltpu.make_async_remote_copy(
            src_ref=src, dst_ref=dst, send_sem=send_sem.at[at], recv_sem=recv_sem.at[at],
            device_id=(peer,), device_id_type=MESH,
        ).start()

    def settle(ref, sem):
        pltpu.make_async_copy(ref, ref, sem).wait()

    def flips(bits):
        steps = []
        for bit in bits:
            steps.append(bit - 2 * bit * lax.rem(lax.div(me, bit), 2))
        return steps

    low_bits = [1, 2, 4]
    high_bits = [8 << k for k in range((n // 8).bit_length() - 1)]
    low_steps, high_steps = flips(low_bits), flips(high_bits)

    def to_peers(send):
        def eight(base, first):
            for k in range(first, 8):
                peer = base
                for bit, step in zip(low_bits, low_steps):
                    if k & bit:
                        peer = peer + step
                send(peer)

        def block_of(c, carry):
            base = me
            for k, step in enumerate(high_steps):
                base = base + step * lax.rem(lax.div(c, 1 << k), 2)
            eight(base, 0)
            return carry

        eight(me, 1)
        lax.fori_loop(1, n // 8, block_of, 0)

    def send_meta(peer):
        post(meta.at[peer], meta_in.at[me], peer, META)

    def send_first(peer):
        post(send_a.at[:, peer], recv.at[pl.ds(near, late), me], peer, A)

    def send_second(first, size):
        lines = pl.ds(first, size)

        def send(peer):
            post(send_b.at[lines, peer], recv.at[lines, me], peer, B)

        return send

    def spread(ref, source):
        def one(k, carry):
            other = lax.rem(inside + k, members)
            post(ref.at[:, other], recv.at[pl.ds(direct, extra), source], level * members + other, X)
            return carry
        lax.fori_loop(1, members, one, 0)

    far_message, near_message = pl.ds(0, pool + 1), pl.ds(0, small + 1)
    beside_dev = beside * members + inside
    across_dev = across * members + inside
    corner_dev = corner * members + inside

    post(far_out.at[far_message], far_in.at[far_message], across_dev, FAR)
    post(near_out.at[near_message], near_in.at[near_message], beside_dev, NEAR)
    to_peers(send_meta)
    load_rot.wait()
    load_cent.start()

    def halve(t, carry):
        at = pl.ds(pl.multiple_of(t * LANES, LANES), LANES)
        hi, lo = split(rot_buf[at, :])
        rot_hi[at, :] = hi
        rot_lo[at, :] = lo
        return carry

    lax.fori_loop(0, width // LANES, halve, 0)

    def turn_rows(rows):
        both, top = pl.ds(0, 2 * rows), pl.ds(0, rows)

        def turned(t, carry):
            at = pl.ds(pl.multiple_of(t * 256, 256), 256)
            value = dot(left[both, :], rot_hi[:, at])
            hi, lo = split(value[:rows] + value[rows:] + dot(left[top, :], rot_lo[:, at]))
            turned_hi[top, at] = hi
            turned_lo[top, at] = lo
            return carry

        lax.fori_loop(0, width // 256, turned, 0)

    turn_rows(count)
    base_x = late * n
    base_b = base_x + extra * members
    wanted = base_b + near * n
    table = lax.broadcasted_iota(jnp.int32, (wanted, LANES), 0)
    picks = []
    for r in range(parts):
        owner, slot = owner_of[r], slot_of[r]
        spot = (slot - direct) * members + lax.rem(owner, members)
        target = jnp.where(slot < direct, (slot - near) * n + owner, -1)
        target = jnp.where(slot < near, base_b + slot * n + owner, target)
        target = jnp.where(home[r], base_x + spot, target)
        picks.append(hot(table == target))
    pick = jnp.concatenate(picks, axis=1)
    for b in range(0, tall, 2):
        cols = pl.ds(b * LANES, 2 * LANES)
        value = dot(pick, turned_hi[:, cols]) + dot(pick, turned_lo[:, cols])
        for h in range(2):
            got = value[:, h * LANES:(h + 1) * LANES]
            send_a_f[pl.ds(b + h, late * n, stride=tall), :] = got[:base_x]
            send_x_f[pl.ds(b + h, extra * members, stride=tall), :] = got[base_x:base_b]
            send_b_f[pl.ds(b + h, near * n, stride=tall), :] = got[base_b:]
    to_peers(send_first)
    spread(send_x, me)
    to_peers(send_second(0, soon))
    for s in range(late):
        recv_f[tile_of((near + s) * n + me), :] = send_a_f[tile_of(s * n + me), :]
    for s in range(near):
        recv_f[tile_of(s * n + me), :] = send_b_f[tile_of(s * n + me), :]
    for s in range(extra):
        recv_f[tile_of((direct + s) * n + me), :] = send_x_f[tile_of(s * members + inside), :]

    keep_emb = pltpu.make_async_copy(emb, emb_out, load_sem.at[5])
    keep_emb.start()
    span_meta = meta_in.at[pl.ds(0, n - 1)]
    settle(span_meta, recv_sem.at[META])

    got = meta_in[:, 0, :]
    if n < LANES:
        got = jnp.concatenate([got, jnp.zeros((LANES - n, LANES), jnp.int32)], axis=0)
    fields = jnp.transpose(got)
    most_out[...] = jnp.broadcast_to(jnp.max(fields[2 * real:2 * real + 1, :], axis=1, keepdims=True), (1, LANES))
    per = LANES // n
    rolled = [fields if k == 0 else pltpu.roll(fields, n * k, 1) for k in range(per)]

    def row_of(g, first):
        total = jnp.zeros((1, LANES), jnp.int32)
        for k in range(per):
            at = first + g * per + k
            total = total + rolled[k][at:at + 1, :]
        return total

    list_row, key_row, key_col, list_col, id_col = [], [], [], [], []
    for g in range(groups):
        found = row_of(g, 0) - 1
        safe = jnp.where(found >= 0, found, owned)
        entry = g * LANES + lane
        key = safe * entries + lax.rem(entry, n) * real + lax.div(entry, n)
        list_row.append(safe)
        key_row.append(key)
        key_col.append(column_of(key))
        list_col.append(column_of(safe))
        id_col.append(column_of(row_of(g, real)))

    slot_at = lax.broadcasted_iota(jnp.int32, (cap, LANES), 0)
    slot_list = jnp.zeros((cap, LANES), jnp.int32)
    pos_col = []
    for g in range(groups):
        rank = jnp.zeros((1, LANES), jnp.int32)
        for h in range(groups):
            less = (key_col[h] < key_row[g]).astype(jnp.int32)
            rank = rank + jnp.sum(less, axis=0, keepdims=True)
        rank = jnp.where(list_row[g] < owned, rank, cap + entries)
        hit = slot_at == rank
        place[:, pl.ds(g * LANES, LANES)] = hot(hit)
        slot_list = slot_list + jnp.where(hit, list_row[g] + 1, 0)
        pos_col.append(column_of(rank))
    at_list = jnp.sum(slot_list, axis=1, keepdims=True) - 1

    def piece(ref, first, rows, b):
        return ref[pl.ds(first * tall + b, rows, stride=tall), :]

    def pair(ref, first, rows, b):
        return split(jnp.concatenate([piece(ref, first, rows, b), piece(ref, first, rows, b + 1)], axis=1))

    def expand(source, rows, used, targets):
        high = len(targets) * extra * members
        code = source[pl.ds(used * tall, 1), :][:, :rows].astype(jnp.int32)
        choose = hot(lax.broadcasted_iota(jnp.int32, (high, rows), 0) == code)
        for b in range(0, tall, 2):
            cols = pl.ds(b * LANES, 2 * LANES)
            hi, lo = pair(source, 0, rows, b)
            left[pl.ds(0, rows), cols] = hi
            left[pl.ds(rows, rows), cols] = lo
        turn_rows(rows)
        for b in range(0, tall, 2):
            cols = pl.ds(b * LANES, 2 * LANES)
            value = dot(choose, turned_hi[pl.ds(0, rows), cols]) + dot(choose, turned_lo[pl.ds(0, rows), cols])
            for k, target in enumerate(targets):
                for h in range(2):
                    part = value[k * extra * members:(k + 1) * extra * members, h * LANES:(h + 1) * LANES]
                    target[pl.ds(b + h, extra * members, stride=tall), :] = part

    def keep(ref, source):
        for s in range(extra):
            recv_f[tile_of((direct + s) * n + source), :] = ref[tile_of(s * members + inside), :]

    settle(near_in.at[near_message], recv_sem.at[NEAR])
    expand(near_in_f, block_near, small, [part_1_f])
    spread(part_1, beside_dev)
    keep(part_1_f, beside_dev)

    settle(far_in.at[far_message], recv_sem.at[FAR])
    expand(far_in_f, block, pool, [part_2_f, part_3_f])

    def send_over(k, carry):
        other = lax.rem(inside + k, members)
        post(part_3.at[:, other], recv.at[pl.ds(direct, extra), across_dev], beside * members + other, X)
        return carry

    lax.fori_loop(0, members, send_over, 0)
    spread(part_2, across_dev)
    keep(part_2_f, across_dev)
    if near > soon:
        to_peers(send_second(soon, near - soon))

    for q in range(cap // LANES):
        total = jnp.zeros((1, LANES), jnp.int32)
        for g in range(groups):
            hit = pos_col[g] == lane + q * LANES
            total = total + jnp.sum(jnp.where(hit, id_col[g] + 1, 0), axis=0, keepdims=True)
        ids_out[pl.ds(q, 1), :] = total - 1
    for q in range(owned // LANES):
        total = jnp.zeros((1, LANES), jnp.int32)
        for g in range(groups):
            less = (list_col[g] < lane + q * LANES).astype(jnp.int32)
            total = total + jnp.sum(less, axis=0, keepdims=True)
        off_out[pl.ds(q, 1), :] = total

    res[...] = jnp.zeros_like(res)
    load_cent.wait()
    step = 256

    def centre(t, carry):
        base = pl.multiple_of(t * step, step)
        table = lax.broadcasted_iota(jnp.int32, (cap, step), 1) + base
        pick = hot(table == at_list)
        for c in range(width // step):
            cols = pl.ds(c * step, step)
            hi, lo = split(cent_buf[pl.ds(base, step), cols])
            res[:, cols] -= dot(pick, hi) + dot(pick, lo)
        return carry

    lax.fori_loop(0, owned // step, centre, 0)

    for b in range(0, tall, 2):
        cols = pl.ds(b * LANES, 2 * LANES)
        hi, lo = split(res[:, cols])
        left[pl.ds(0, cap), cols] = hi
        left[pl.ds(cap, cap), cols] = lo

    def tile(t, carry):
        at = pl.ds(pl.multiple_of(t * 256, 256), 256)
        r_hi = rot_hi[:, at]
        top, low = left[pl.ds(0, cap), :], left[pl.ds(cap, cap), :]
        out[:, at] = dot(top, r_hi) + dot(low, r_hi) + dot(top, rot_lo[:, at])
        return carry

    lax.fori_loop(0, width // 256, tile, 0)

    rest = entries - near * n
    place_twice[:, :rest] = place[:, near * n:]
    place_twice[:, rest:] = place[:, near * n:]
    span_a = recv.at[pl.ds(near, late), pl.ds(0, n - 1)]
    settle(span_a, recv_sem.at[A])
    span_x = recv_f.at[pl.ds(0, extra * (LEVELS * members - LEVELS + 1) * tall)]
    settle(span_x, recv_sem.at[X])
    for b in range(0, tall, 2):
        cols = pl.ds(b * LANES, 2 * LANES)
        hi, lo = pair(recv_f, near * n, rest, b)
        out[:, cols] += dot(place_twice[...], jnp.concatenate([hi, lo], axis=0))

    span_b = recv.at[pl.ds(0, near), pl.ds(0, n - 1)]
    last_place[:, :near * n] = place[:, :near * n]
    last_place[:, near * n:] = place[:, :near * n]
    settle(span_b, recv_sem.at[B])
    for b in range(0, tall, 2):
        cols = pl.ds(b * LANES, 2 * LANES)
        hi, lo = pair(recv_f, 0, near * n, b)
        last[pl.ds(0, near * n), cols] = hi
        last[pl.ds(near * n, near * n), cols] = lo

    keep_emb.wait()
    settle(span_meta, send_sem.at[META])
    settle(span_a, send_sem.at[A])
    settle(span_b, send_sem.at[B])
    settle(span_x, send_sem.at[X])
    settle(far_in.at[far_message], send_sem.at[FAR])
    settle(near_in.at[near_message], send_sem.at[NEAR])


def finish_kernel(pool, most, rows, last, place, ids, offsets, rows_out, ids_out, off_out, buf, sem):
    wide = 256
    tiles = rows.shape[1] // wide
    moves = [
        pltpu.make_async_copy(ids, ids_out, sem.at[tiles]),
        pltpu.make_async_copy(offsets, off_out, sem.at[tiles + 1]),
    ]
    for move in moves:
        move.start()
    for t in range(tiles):
        cols = pl.ds(t * wide, wide)
        kept = rows[:, cols]
        buf[t] = jnp.where(most[0:1, 0:1] > pool, kept, kept + dot(place[...], last[:, cols]))
        move = pltpu.make_async_copy(buf.at[t], rows_out.at[:, cols], sem.at[t])
        move.start()
        moves.append(move)
    for move in moves:
        move.wait()


def finish(pool, most, rows, last, place, ids, offsets):
    vmem = pl.BlockSpec(memory_space=pltpu.VMEM)
    hbm = pl.BlockSpec(memory_space=pltpu.HBM)
    cap, width = rows.shape
    return pl.pallas_call(
        functools.partial(finish_kernel, pool),
        out_shape=tuple(jax.ShapeDtypeStruct(x.shape, x.dtype) for x in (rows, ids, offsets)),
        in_specs=[vmem] * 6,
        out_specs=(hbm,) * 3,
        scratch_shapes=[pltpu.VMEM((width // 256, cap, 256), F32), pltpu.SemaphoreType.DMA((width // 256 + 2,))],
        compiler_params=pltpu.CompilerParams(vmem_limit_bytes=8 * 1024 * 1024),
    )(most, rows, last, place, ids, offsets)


LEVELS = 4
POOL = 44
SMALL = 34


def local(embeddings, lists, row_ids, centroids, rotation):
    row_count, width = embeddings.shape
    owned = centroids.shape[0]
    n = lax.axis_size("dev")
    cap = 2 * row_count
    real = cap // n
    near = LANES // n
    direct = (7 * real + 8) // 16
    late, extra = direct - near, real - direct
    members = n // LEVELS
    pool, small = POOL, SMALL
    block, block_near = -(-(pool + 1) // 16) * 16, -(-(small + 1) // 16) * 16
    tall = width // LANES
    by_lane = (row_count // LANES, LANES)
    vmem = pl.BlockSpec(memory_space=pltpu.VMEM)
    hbm = pl.BlockSpec(memory_space=pltpu.HBM)

    def rows_of(*lead):
        return pltpu.VMEM((*lead, tall, LANES), F32)

    packed, last, place, ids, offsets, most, copied = pl.pallas_call(
        functools.partial(relayed_kernel, n, real, near, direct, pool, small),
        out_shape=(
            jax.ShapeDtypeStruct((cap, width), F32),
            jax.ShapeDtypeStruct((2 * near * n, width), BF16),
            jax.ShapeDtypeStruct((cap, 2 * near * n), BF16),
            jax.ShapeDtypeStruct((cap // LANES, LANES), jnp.int32),
            jax.ShapeDtypeStruct((owned // LANES, LANES), jnp.int32),
            jax.ShapeDtypeStruct((1, LANES), jnp.int32),
            jax.ShapeDtypeStruct((row_count, width), F32),
        ),
        in_specs=[hbm] * 5,
        out_specs=(vmem,) * 6 + (hbm,),
        scratch_shapes=[
            pltpu.VMEM((row_count, width), F32),
            pltpu.VMEM(by_lane, jnp.int32),
            pltpu.VMEM(by_lane, jnp.int32),
            pltpu.VMEM((row_count, width), BF16),
            pltpu.VMEM((row_count, width), BF16),
            rows_of(late, n), rows_of(near, n), rows_of(extra, members), rows_of(block), rows_of(block_near),
            pltpu.VMEM((n, 1, LANES), jnp.int32),
            rows_of(real, n), rows_of(block), rows_of(block_near),
            pltpu.VMEM((n, 1, LANES), jnp.int32),
            rows_of(extra, members), rows_of(extra, members), rows_of(extra, members),
            pltpu.VMEM((owned, width), F32),
            pltpu.VMEM((width, width), F32),
            pltpu.VMEM((width, width), BF16),
            pltpu.VMEM((width, width), BF16),
            pltpu.VMEM((cap, width), F32),
            pltpu.VMEM((2 * cap, width), BF16),
            pltpu.VMEM((cap, n * real), BF16),
            pltpu.VMEM((cap, 2 * (n * real - near * n)), BF16),
            pltpu.SemaphoreType.DMA((6,)),
            pltpu.SemaphoreType.DMA((6,)),
            pltpu.SemaphoreType.DMA((6,)),
        ],
        compiler_params=pltpu.CompilerParams(
            collective_id=0, has_side_effects=True, vmem_limit_bytes=55200000
        ),
    )(embeddings, lists.reshape(by_lane), row_ids.reshape(by_lane), centroids, rotation)
    packed = lax.cond(
        most[0, 0] > pool,
        lambda: full(copied, lists, row_ids, centroids, rotation),
        lambda: packed,
    )
    packed, ids, offsets = finish(pool, most, packed, last, place, ids, offsets)
    return packed, ids.reshape(-1), offsets.reshape(-1)


def solution(mesh):
    in_specs = (P("dev", None), P("dev"), P("dev"), P("dev", None), P())
    out_specs = (P("dev", None), P("dev"), P("dev"))
    return jax.shard_map(local, mesh=mesh, in_specs=in_specs, out_specs=out_specs, check_vma=False)
```
